16 devices in a mesh: stage: 4 (over z, y), expert: 4 (over x, core).
Axes of the slice: x: 2, y: 2, z: 2, core: 2. Of those that a mesh axis runs over, the one named last changes fastest.
Arguments:
- w_gate: bfloat16 [8, 4, 2048, 768], P('stage', 'expert')
- w_up: bfloat16 [8, 4, 2048, 768], P('stage', 'expert')
- w_down: bfloat16 [8, 4, 768, 2048], P('stage', 'expert')
- dense: bfloat16 [8, 2048, 4096], P('stage')
- hot_ids: int32 [2], replicated
- spare_map: int32 [16], P(('stage', 'expert'))
Outputs:
- output 1: bfloat16 [8, 16, 2048, 384], P(None, ('stage', 'expert'))
- output 2: bfloat16 [8, 16, 192, 2048], P(None, ('stage', 'expert'))
- output 3: bfloat16 [8, 2048, 4096], replicated
- output 4: bfloat16 [8, 16, 2048, 384], P(None, ('stage', 'expert'))
- output 5: bfloat16 [8, 16, 192, 2048], P(None, ('stage', 'expert'))
All inputs are finite; a program needn't handle non-finite values.
Results may differ from the reference program's by a relative error of at most 0.001.
Values are sent between devices in bfloat16 or wider.
A program may use at most 1 GiB of HBM per device.

```python
import jax
import jax.numpy as jnp

LAYERS = 8
EXPERTS = 4
D_MODEL = 2048
FF_WIDTH = 768
DENSE_WIDTH = 4096
PIECES = 4
STAGES = 4
GROUPS = 4
DEVICES = 16
HOT_UNITS = 2

PIECE_WIDTH = FF_WIDTH // PIECES
UNIT_COUNT = EXPERTS * PIECES
PER_DEVICE = UNIT_COUNT // DEVICES


def draw_placement(base_key):
    key_list = jax.random.split(base_key, 6)
    first_dev = jax.random.randint(key_list[0], (), 0, DEVICES, dtype=jnp.int32)
    shift_stage = jax.random.randint(key_list[1], (), 1, STAGES, dtype=jnp.int32)
    shift_group = jax.random.randint(key_list[2], (), 1, GROUPS, dtype=jnp.int32)
    second_stage = (first_dev // GROUPS + shift_stage) % STAGES
    second_group = (first_dev % GROUPS + shift_group) % GROUPS
    second_dev = second_stage * GROUPS + second_group
    offsets = jax.random.randint(key_list[3], (HOT_UNITS,), 0, PER_DEVICE, dtype=jnp.int32)
    hot_ids = jnp.stack([first_dev, second_dev]) * PER_DEVICE + offsets
    base_map = jax.random.randint(key_list[4], (DEVICES,), -1, HOT_UNITS, dtype=jnp.int32)
    slot_order = jax.random.permutation(key_list[5], DEVICES)
    forced = jnp.concatenate([jnp.arange(HOT_UNITS, dtype=jnp.int32), jnp.full((1,), -1, dtype=jnp.int32)])
    spare_map = base_map.at[slot_order[:HOT_UNITS + 1]].set(forced)
    return hot_ids.astype(jnp.int32), spare_map.astype(jnp.int32)


def setup_inputs(seed: int = 0) -> dict:
    key_list = jax.random.split(jax.random.key(seed), 5)
    expert_shape = (LAYERS, EXPERTS, D_MODEL, FF_WIDTH)
    w_gate = jax.random.normal(key_list[0], expert_shape, jnp.float32).astype(jnp.bfloat16)
    w_up = jax.random.normal(key_list[1], expert_shape, jnp.float32).astype(jnp.bfloat16)
    w_down = jax.random.normal(key_list[2], (LAYERS, EXPERTS, FF_WIDTH, D_MODEL), jnp.float32).astype(jnp.bfloat16)
    dense = jax.random.normal(key_list[3], (LAYERS, D_MODEL, DENSE_WIDTH), jnp.float32).astype(jnp.bfloat16)
    hot_ids, spare_map = draw_placement(key_list[4])
    return {'w_gate': w_gate, 'w_up': w_up, 'w_down': w_down, 'dense': dense, 'hot_ids': hot_ids, 'spare_map': spare_map}


def reference(w_gate, w_up, w_down, dense, hot_ids, spare_map):
    gate_parts = w_gate.reshape(LAYERS, EXPERTS, D_MODEL, PIECES, PIECE_WIDTH)
    up_parts = w_up.reshape(LAYERS, EXPERTS, D_MODEL, PIECES, PIECE_WIDTH)
    gate_up = jnp.concatenate([gate_parts, up_parts], axis=-1)
    gate_up = jnp.transpose(gate_up, (0, 1, 3, 2, 4)).reshape(LAYERS, UNIT_COUNT, D_MODEL, 2 * PIECE_WIDTH)
    down_units = w_down.reshape(LAYERS, UNIT_COUNT, PIECE_WIDTH, D_MODEL)
    hot_gate_up = jnp.take(gate_up, hot_ids, axis=1)
    hot_down = jnp.take(down_units, hot_ids, axis=1)
    slot_index = jnp.maximum(spare_map, 0)
    filled = (spare_map >= 0)[None, :, None, None]
    spare_gate_up = jnp.where(filled, jnp.take(hot_gate_up, slot_index, axis=1), jnp.zeros((), gate_up.dtype))
    spare_down = jnp.where(filled, jnp.take(hot_down, slot_index, axis=1), jnp.zeros((), down_units.dtype))
    return gate_up, down_units, dense, spare_gate_up, spare_down
```

```python
import functools

import jax
import jax.numpy as jnp
from jax import lax
from jax.experimental import pallas as pl
from jax.experimental.pallas import tpu as pltpu
from jax.sharding import PartitionSpec as P


MESH = pl.DeviceIdType.MESH
ANY = pl.BlockSpec(memory_space=pl.ANY)
SMEM = pl.BlockSpec(memory_space=pltpu.SMEM)
BF16 = jnp.bfloat16

LAYERS, HIDDEN, WIDTH, DENSE = 2, 2048, 768, 4096
PIECES, PIECE = 4, 192
STAGES = 4
HOT = 2
LANES = 128
HOT13 = 3 * HIDDEN
HOT_ROWS = HOT13 + 16 * PIECE
DENSE_CHUNKS = 16
DENSE_CHUNK = 1024 // DENSE_CHUNKS
DIRECT = 3
HOT_CHUNKS = 4
HOT_CHUNK = HOT_ROWS // HOT_CHUNKS
PACK_STEPS = 4


def loop(count, body):
    def step(k, carry):
        body(k)
        return carry

    lax.fori_loop(0, count, step, 0)


def pack_kernel(pos_ref, ids_ref, gate, up, down, *outs):
    out13, out2, hot = outs[:4], outs[4:8], outs[8]
    stage = pos_ref[0]
    rows = HIDDEN // PACK_STEPS
    cols = HIDDEN // PACK_STEPS
    blocks = cols // LANES
    step = pl.program_id(1)
    for here in range(STAGES):
        @pl.when(stage == here)
        def _():
            for r in range(PIECES):
                p = (here + r) % PIECES
                lo, hi = p * PIECE, (p + 1) * PIECE
                out13[r][0] = jnp.concatenate([gate[0, :, lo:hi], up[0, :, lo:hi]], axis=-1)
                out2[r][0] = down[0, lo:hi, :]
    for h in range(HOT):
        piece = lax.rem(ids_ref[h], PIECES)
        for p in range(PIECES):
            @pl.when(piece == p)
            def _():
                lo, hi = p * PIECE, (p + 1) * PIECE
                unit = jnp.concatenate([gate[0, :, lo:hi], up[0, :, lo:hi]], axis=-1)
                for b in range(3):
                    start = pl.multiple_of(b * HIDDEN + step * rows, rows)
                    hot[h, 0, pl.ds(start, rows), :] = unit[:, b * LANES:(b + 1) * LANES]
                for b in range(blocks):
                    start = pl.multiple_of(HOT13 + (step * blocks + b) * PIECE, PIECE)
                    hot[h, 0, pl.ds(start, PIECE), :] = down[0, lo:hi, b * LANES:(b + 1) * LANES]


def pack(stage, hot_ids, gate, up, down):
    rows = HIDDEN // PACK_STEPS
    wide = pl.BlockSpec((1, rows, WIDTH), lambda l, i, *_: (l, i, 0))
    outs = [pl.BlockSpec((1, rows, 2 * PIECE), lambda l, i, *_: (l, i, 0))] * PIECES
    outs += [pl.BlockSpec((1, PIECE, rows), lambda l, i, *_: (l, 0, i))] * PIECES
    outs += [pl.BlockSpec((HOT, 1, HOT_ROWS, LANES), lambda l, i, *_: (0, l, 0, 0))]
    shapes = [jax.ShapeDtypeStruct((LAYERS, HIDDEN, 2 * PIECE), BF16)] * PIECES
    shapes += [jax.ShapeDtypeStruct((LAYERS, PIECE, HIDDEN), BF16)] * PIECES
    shapes += [jax.ShapeDtypeStruct((HOT, LAYERS, HOT_ROWS, LANES), BF16)]
    return pl.pallas_call(
        pack_kernel,
        grid_spec=pltpu.PrefetchScalarGridSpec(
            num_scalar_prefetch=2,
            grid=(LAYERS, PACK_STEPS),
            in_specs=[wide, wide, pl.BlockSpec((1, WIDTH, rows), lambda l, i, *_: (l, 0, i))],
            out_specs=outs,
        ),
        out_shape=shapes,
        compiler_params=pltpu.CompilerParams(vmem_limit_bytes=48 << 20),
        cost_estimate=pl.CostEstimate(flops=1 << 26, bytes_accessed=45 << 20, transcendentals=0),
        name="pack",
    )(stage, hot_ids, gate, up, down)


def spread_kernel(dense, hotc, ids, full, hotf, cbuf, pbuf, xbuf, ds, dr, hs, hr, es, er, ls):
    stage, expert = lax.axis_index('stage'), lax.axis_index('expert')
    z, y = stage // 2, stage % 2
    x, c = expert // 2, expert % 2
    to_y = (z * 2 + 1 - y, expert)
    to_z = ((1 - z) * 2 + y, expert)
    to_x = (stage, (1 - x) * 2 + c)
    to_p = (stage, x * 2 + 1 - c)
    at_y, at_z, at_yz = z * 2 + 1 - y, (1 - z) * 2 + y, (1 - z) * 2 + 1 - y
    flows = [(at_y, x), (at_z, 1 - x), (at_yz, 1 - x), (at_yz, x), (at_y, 1 - x), (at_z, x)]

    def remote(src, dst, send, recv, to):
        return pltpu.make_async_remote_copy(
            src_ref=src, dst_ref=dst, send_sem=send, recv_sem=recv, device_id=to, device_id_type=MESH)

    def dense_rows(st, half, core, k):
        start = st * 4096 + half * 2048 + core * 1024 + k * DENSE_CHUNK
        return full.at[pl.ds(pl.multiple_of(start, DENSE_CHUNK), DENSE_CHUNK)]

    def hot_rows(st, half, core, k):
        return hotf.at[st, half, core, pl.ds(pl.multiple_of(k * HOT_CHUNK, HOT_CHUNK), HOT_CHUNK)]

    def dense_send(src, dst, flow, k, to):
        return remote(src, dst, ds.at[flow, k], dr.at[flow, k], to)

    def hot_send(src, dst, flow, k, to):
        return remote(src, dst, hs.at[flow, k], hr.at[flow, k], to)

    def dense_own(half, k):
        start = half * 2048 + c * 1024 + k * DENSE_CHUNK
        return dense.at[pl.ds(pl.multiple_of(start, DENSE_CHUNK), DENSE_CHUNK)]

    def dense_on(i, flow, k, to):
        ref = dense_rows(*flows[i], c, k)
        return dense_send(ref, ref, flow, k, to)

    def hot_on(i, flow, k, to):
        ref = hot_rows(*flows[i], c, k)
        return hot_send(ref, ref, flow, k, to)

    def dense_arrival(flow, k):
        ref = dense_rows(*flows[flow % 6], c if flow < 6 else 1 - c, k)
        return dense_send(ref, ref, flow, k, to_p)

    def hot_arrival(flow, k):
        ref = hot_rows(*flows[flow % 6], c if flow < 6 else 1 - c, k)
        return hot_send(ref, ref, flow, k, to_p)

    swap = [remote(hotc.at[h, 1 - c], pbuf.at[h], es.at[h], er.at[h], to_p) for h in range(HOT)]
    load = [pltpu.make_async_copy(hotc.at[h, c], cbuf.at[h], ls.at[h]) for h in range(HOT)]
    for h in range(HOT):
        swap[h].start()
        load[h].start()

    def own(k):
        dense_send(dense_own(x, k), dense_rows(stage, x, c, k), 0, k, to_y).start()
        dense_send(dense_own(1 - x, k), dense_rows(stage, 1 - x, c, k), 1, k, to_z).start()

    loop(DENSE_CHUNKS, own)

    def own_direct(k):
        dense_send(dense_own(1 - x, k), dense_rows(stage, 1 - x, c, k), 4, k, to_y).start()
        dense_send(dense_own(x, k), dense_rows(stage, x, c, k), 5, k, to_z).start()

    loop(DIRECT, own_direct)

    def choose(h, here, other):
        def rows(i):
            at = pl.ds(pl.multiple_of(i * 512, 512), 512)
            cbuf[h, at, :] = jnp.where(here, cbuf[h, at, :], other[h, at, :])

        loop(HOT_ROWS // 512, rows)

    cross = [remote(cbuf.at[h], xbuf.at[h], es.at[2 + h], er.at[2 + h], to_x) for h in range(HOT)]
    for h in range(HOT):
        load[h].wait()
        swap[h].wait_recv()
        choose(h, lax.shift_right_logical(ids[h], 2) == expert, pbuf)
    for h in range(HOT):
        cross[h].start()

    def relay(k, over_x):
        dense_arrival(0, k).wait_recv()
        dense_on(0, 3, k, to_z).start()
        if over_x:
            dense_on(0, 4, k, to_x).start()
        dense_on(0, 6, k, to_p).start()
        dense_arrival(1, k).wait_recv()
        dense_on(1, 2, k, to_y).start()
        if over_x:
            dense_on(1, 5, k, to_x).start()
        dense_on(1, 7, k, to_p).start()

    loop(DIRECT, lambda k: relay(k, False))
    half_way = DENSE_CHUNKS // 2
    loop(half_way - DIRECT, lambda k: relay(k + DIRECT, True))

    for h in range(HOT):
        cross[h].wait()
        choose(h, lax.shift_right_logical(ids[h], 3) == x, xbuf)
    keep = [pltpu.make_async_copy(cbuf.at[h], hotf.at[stage, h, c], ls.at[2 + h]) for h in range(HOT)]
    give = [remote(cbuf.at[h], hotf.at[stage, h, c], es.at[4 + h], er.at[4 + h], to_p) for h in range(HOT)]
    for h in range(HOT):
        keep[h].start()
        give[h].start()

    def hot_own(k):
        at = pl.ds(pl.multiple_of(k * HOT_CHUNK, HOT_CHUNK), HOT_CHUNK)
        hot_send(cbuf.at[x, at], hot_rows(stage, x, c, k), 0, k, to_y).start()
        hot_send(cbuf.at[1 - x, at], hot_rows(stage, 1 - x, c, k), 1, k, to_z).start()

    loop(HOT_CHUNKS, hot_own)
    loop(DENSE_CHUNKS - half_way, lambda k: relay(k + half_way, True))

    def hot_relay(k):
        hot_arrival(0, k).wait_recv()
        hot_on(0, 3, k, to_z).start()
        hot_on(0, 4, k, to_x).start()
        hot_on(0, 6, k, to_p).start()
        hot_arrival(1, k).wait_recv()
        hot_on(1, 2, k, to_y).start()
        hot_on(1, 5, k, to_x).start()
        hot_on(1, 7, k, to_p).start()

    loop(HOT_CHUNKS, hot_relay)

    def dense_last(k):
        for i in (4, 5, 2, 3):
            dense_arrival(i, k).wait_recv()
            dense_on(i, 6 + i, k, to_p).start()

    loop(DENSE_CHUNKS, dense_last)

    def hot_last(k):
        for i in (4, 5, 2, 3):
            hot_arrival(i, k).wait_recv()
            hot_on(i, 6 + i, k, to_p).start()

    loop(HOT_CHUNKS, hot_last)

    def dense_end(k):
        for i in range(12):
            if i >= 6:
                dense_arrival(i, k).wait_recv()
            dense_arrival(i, k).wait_send()

    def hot_end(k):
        for i in range(12):
            if i >= 6:
                hot_arrival(i, k).wait_recv()
            hot_arrival(i, k).wait_send()

    loop(DENSE_CHUNKS, dense_end)
    loop(HOT_CHUNKS, hot_end)
    for h in range(HOT):
        swap[h].wait_send()
        keep[h].wait()
        give[h].wait()


def spread(dense, hotc, hot_ids):
    sem = pltpu.SemaphoreType.DMA
    return pl.pallas_call(
        spread_kernel,
        out_shape=[
            jax.ShapeDtypeStruct((STAGES * 4096, DENSE), BF16),
            jax.ShapeDtypeStruct((STAGES, HOT, LAYERS, HOT_ROWS, LANES), BF16),
        ],
        in_specs=[ANY, ANY, SMEM],
        out_specs=[ANY, ANY],
        scratch_shapes=[pltpu.VMEM((HOT, HOT_ROWS, LANES), BF16)] * 3 + [
            sem((12, DENSE_CHUNKS)), sem((12, DENSE_CHUNKS)),
            sem((12, HOT_CHUNKS)), sem((12, HOT_CHUNKS)),
            sem((6,)), sem((6,)), sem((4,)),
        ],
        compiler_params=pltpu.CompilerParams(has_side_effects=True, vmem_limit_bytes=48 << 20),
        cost_estimate=pl.CostEstimate(flops=1 << 32, bytes_accessed=256 << 20, transcendentals=0),
        name="spread",
    )(dense, hotc, hot_ids)


COPY_ROWS = 256
COPY_SLOTS = 12


def dense_copy_kernel(pos, dense, full, out, buf, rs, ws):
    count = STAGES * 4096 // COPY_ROWS
    per_stage = 4096 // COPY_ROWS
    stage = pos[0]

    def rows(k):
        return pl.ds(pl.multiple_of(k * COPY_ROWS, COPY_ROWS), COPY_ROWS)

    def read(k, ref, at):
        slot = lax.rem(k, COPY_SLOTS)
        return pltpu.make_async_copy(ref.at[rows(at)], buf.at[slot], rs.at[slot])

    def write(k):
        slot = lax.rem(k, COPY_SLOTS)
        return pltpu.make_async_copy(buf.at[slot], out.at[rows(k)], ws.at[slot])

    def start(k):
        mine = k // per_stage == stage

        @pl.when(mine)
        def _():
            read(k, dense, k - stage * per_stage).start()

        @pl.when(jnp.logical_not(mine))
        def _():
            read(k, full, k).start()

    ahead = COPY_SLOTS // 2
    loop(ahead, start)

    def step(k):
        @pl.when(k + ahead < count)
        def _():
            @pl.when(k + ahead >= COPY_SLOTS)
            def _():
                write(k + ahead - COPY_SLOTS).wait()

            start(k + ahead)

        read(k, full, k).wait()
        write(k).start()

    loop(count, step)
    loop(COPY_SLOTS, lambda k: write(count - COPY_SLOTS + k).wait())


def dense_copy(stage, dense, full):
    return pl.pallas_call(
        dense_copy_kernel,
        out_shape=jax.ShapeDtypeStruct((STAGES * 4096, DENSE), BF16),
        in_specs=[SMEM, ANY, ANY],
        out_specs=ANY,
        scratch_shapes=[
            pltpu.VMEM((COPY_SLOTS, COPY_ROWS, DENSE), BF16),
            pltpu.SemaphoreType.DMA((COPY_SLOTS,)), pltpu.SemaphoreType.DMA((COPY_SLOTS,)),
        ],
        compiler_params=pltpu.CompilerParams(vmem_limit_bytes=48 << 20),
        cost_estimate=pl.CostEstimate(flops=1 << 28, bytes_accessed=256 << 20, transcendentals=0),
        name="dense_copy",
    )(stage, dense, full)


def spare_kernel(slot, hotf, out13, out2, b13, b2, rs, ws):
    pick = slot[0]
    total = STAGES * LAYERS

    def reads(n, h):
        src = hotf.at[n // LAYERS, h, n % LAYERS]
        for b in range(3):
            yield pltpu.make_async_copy(
                src.at[pl.ds(b * HIDDEN, HIDDEN)], b13.at[n, :, pl.ds(b * LANES, LANES)], rs.at[n])
        for b in range(16):
            yield pltpu.make_async_copy(
                src.at[pl.ds(HOT13 + b * PIECE, PIECE)], b2.at[n, :, pl.ds(b * LANES, LANES)], rs.at[n])

    @pl.when(pick >= 0)
    def _():
        for n in range(total):
            for copy in reads(n, jnp.maximum(pick, 0)):
                copy.start()

    @pl.when(pick < 0)
    def _():
        for n in range(total):
            b13[n] = jnp.zeros((HIDDEN, 2 * PIECE), BF16)
            b2[n] = jnp.zeros((PIECE, HIDDEN), BF16)

    writes = []
    for n in range(total):
        @pl.when(pick >= 0)
        def _():
            pltpu.make_async_copy(out13.at[n], b13.at[n], rs.at[n]).wait()
            pltpu.make_async_copy(out2.at[n], b2.at[n], rs.at[n]).wait()

        writes.append(pltpu.make_async_copy(b13.at[n], out13.at[n], ws.at[n]))
        writes.append(pltpu.make_async_copy(b2.at[n], out2.at[n], ws.at[total + n]))
        writes[-2].start()
        writes[-1].start()
    for copy in writes:
        copy.wait()


def spare(slot, hotf):
    total = STAGES * LAYERS
    return pl.pallas_call(
        spare_kernel,
        out_shape=[
            jax.ShapeDtypeStruct((total, HIDDEN, 2 * PIECE), BF16),
            jax.ShapeDtypeStruct((total, PIECE, HIDDEN), BF16),
        ],
        in_specs=[SMEM, ANY],
        out_specs=[ANY, ANY],
        scratch_shapes=[
            pltpu.VMEM((total, HIDDEN, 2 * PIECE), BF16),
            pltpu.VMEM((total, PIECE, HIDDEN), BF16),
            pltpu.SemaphoreType.DMA((total,)), pltpu.SemaphoreType.DMA((2 * total,)),
        ],
        compiler_params=pltpu.CompilerParams(vmem_limit_bytes=48 << 20),
        cost_estimate=pl.CostEstimate(flops=1 << 26, bytes_accessed=36 << 20, transcendentals=0),
        name="spare",
    )(slot, hotf)


def place_kernel(pos, *refs):
    in13, in2, (out13, out2, b13, b2, rs, ws) = refs[:4], refs[4:8], refs[8:]
    copies = []
    for r in range(PIECES):
        first = lax.rem(pos[0] - r + PIECES, PIECES) * LAYERS
        for j, (src, buf, out) in enumerate(((in13[r], b13, out13), (in2[r], b2, out2))):
            n = 2 * r + j
            copies.append((
                pltpu.make_async_copy(src, buf.at[r], rs.at[n]),
                pltpu.make_async_copy(buf.at[r], out.at[pl.ds(first, LAYERS)], ws.at[n])))
    for read, _ in copies:
        read.start()
    for read, write in copies:
        read.wait()
        write.start()
    for _, write in copies:
        write.wait()


def place(column, parts13, parts2):
    total = STAGES * LAYERS
    return pl.pallas_call(
        place_kernel,
        out_shape=[
            jax.ShapeDtypeStruct((total, HIDDEN, 2 * PIECE), BF16),
            jax.ShapeDtypeStruct((total, PIECE, HIDDEN), BF16),
        ],
        in_specs=[SMEM] + [ANY] * 8,
        out_specs=[ANY, ANY],
        scratch_shapes=[
            pltpu.VMEM((PIECES, LAYERS, HIDDEN, 2 * PIECE), BF16),
            pltpu.VMEM((PIECES, LAYERS, PIECE, HIDDEN), BF16),
            pltpu.SemaphoreType.DMA((2 * PIECES,)), pltpu.SemaphoreType.DMA((2 * PIECES,)),
        ],
        compiler_params=pltpu.CompilerParams(vmem_limit_bytes=48 << 20),
        cost_estimate=pl.CostEstimate(flops=1 << 26, bytes_accessed=36 << 20, transcendentals=0),
        name="place",
    )(column, *parts13, *parts2)


def solution(mesh):
    flat_axes = ('stage', 'expert')

    def rounds(r):
        return [(s * 4 + e, e * 4 + (s + r) % 4) for s in range(4) for e in range(4)]

    def local_move(w_gate, w_up, w_down, dense, hot_ids, spare_map):
        stage = lax.axis_index('stage').astype(jnp.int32)[None]
        column = lax.axis_index('expert').astype(jnp.int32)[None]
        dense = dense.reshape(4096, DENSE)
        *parts, hotc = pack(stage, hot_ids, w_gate[:, 0], w_up[:, 0], w_down[:, 0])
        full, hotf = spread(dense, hotc, hot_ids)
        *parts, full, hotf = lax.optimization_barrier((*parts, full, hotf))
        moved = [lax.ppermute(part, flat_axes, rounds(i % 4)) for i, part in enumerate(parts)]
        dense_out = dense_copy(stage, dense, full).reshape(STAGES * LAYERS, HIDDEN, DENSE)
        spare13, spare2 = spare(spare_map, hotf)
        w13, w2 = place(column, moved[:4], moved[4:])
        return w13[:, None], w2[:, None], dense_out, spare13[:, None], spare2[:, None]

    expert_spec = P('stage', 'expert', None, None)
    unit_spec = P(None, flat_axes, None, None)
    return jax.shard_map(
        local_move,
        mesh=mesh,
        in_specs=(expert_spec, expert_spec, expert_spec, P('stage', None, None), P(None), P(flat_axes)),
        out_specs=(unit_spec, unit_spec, P(None, None, None), unit_spec, unit_spec),
        check_vma=False,
    )
```

```python
import functools

import jax
import jax.numpy as jnp
from jax import lax
from jax.experimental import pallas as pl
from jax.experimental.pallas import tpu as pltpu
from jax.sharding import PartitionSpec as P


MESH = pl.DeviceIdType.MESH
ANY = pl.BlockSpec(memory_space=pl.ANY)
SMEM = pl.BlockSpec(memory_space=pltpu.SMEM)
BF16 = jnp.bfloat16

LAYERS, HIDDEN, WIDTH, DENSE = 2, 2048, 768, 4096
PIECES, PIECE = 4, 192
STAGES = 4
HOT = 2
LANES = 128
HOT13 = 3 * HIDDEN
HOT_ROWS = HOT13 + 16 * PIECE
DENSE_CHUNKS = 32
DENSE_CHUNK = 1024 // DENSE_CHUNKS
DIRECT = 6
HOT_CHUNKS = 4
HOT_CHUNK = HOT_ROWS // HOT_CHUNKS
PACK_STEPS = 4
PACK_ROWS = HIDDEN // PACK_STEPS
SUB_ROWS = 64


def loop(count, body):
    def step(k, carry):
        body(k)
        return carry

    lax.fori_loop(0, count, step, 0)


def spread_kernel(dense, gate, up, down, ids, full, hotf, w2buf, *refs):
    parts, refs = [refs[:4], refs[4:8]], refs[8:]
    gin, uin, din, cut, hot, pbuf, xbuf = refs[:7]
    ds, dr, hs, hr, es, er, ls, ins, outs, ws, wr = refs[7:]
    stage, expert = lax.axis_index('stage'), lax.axis_index('expert')
    z, y = stage // 2, stage % 2
    x, c = expert // 2, expert % 2
    to_y = (z * 2 + 1 - y, expert)
    to_z = ((1 - z) * 2 + y, expert)
    to_x = (stage, (1 - x) * 2 + c)
    to_p = (stage, x * 2 + 1 - c)
    at_y, at_z, at_yz = z * 2 + 1 - y, (1 - z) * 2 + y, (1 - z) * 2 + 1 - y
    flows = [(at_y, x), (at_z, 1 - x), (at_yz, 1 - x), (at_yz, x), (at_y, 1 - x), (at_z, x)]

    def remote(src, dst, send, recv, to):
        return pltpu.make_async_remote_copy(
            src_ref=src, dst_ref=dst, send_sem=send, recv_sem=recv, device_id=to, device_id_type=MESH)

    def dense_rows(st, half, core, k):
        start = st * 4096 + half * 2048 + core * 1024 + k * DENSE_CHUNK
        return full.at[pl.ds(pl.multiple_of(start, DENSE_CHUNK), DENSE_CHUNK)]

    def hot_rows(st, half, core, k):
        return hotf.at[st, half, core, pl.ds(pl.multiple_of(k * HOT_CHUNK, HOT_CHUNK), HOT_CHUNK)]

    def dense_send(src, dst, flow, k, to):
        return remote(src, dst, ds.at[flow, k], dr.at[flow, k], to)

    def hot_send(src, dst, flow, k, to):
        return remote(src, dst, hs.at[flow, k], hr.at[flow, k], to)

    def dense_own(half, k):
        start = half * 2048 + c * 1024 + k * DENSE_CHUNK
        return dense.at[pl.ds(pl.multiple_of(start, DENSE_CHUNK), DENSE_CHUNK)]

    def dense_on(i, flow, k, to):
        ref = dense_rows(*flows[i], c, k)
        return dense_send(ref, ref, flow, k, to)

    def hot_on(i, flow, k, to):
        ref = hot_rows(*flows[i], c, k)
        return hot_send(ref, ref, flow, k, to)

    def dense_arrival(flow, k):
        ref = dense_rows(*flows[flow % 6], c if flow < 6 else 1 - c, k)
        return dense_send(ref, ref, flow, k, to_p)

    def hot_arrival(flow, k):
        ref = hot_rows(*flows[flow % 6], c if flow < 6 else 1 - c, k)
        return hot_send(ref, ref, flow, k, to_p)

    loads = []
    for l in range(LAYERS):
        for i in range(PACK_STEPS):
            at = pl.ds(i * PACK_ROWS, PACK_ROWS)
            trio = ((gate.at[l, at], gin.at[l, at]), (up.at[l, at], uin.at[l, at]),
                    (down.at[l, :, at], din.at[l, :, at]))
            loads.append([
                pltpu.make_async_copy(src, dst, ins.at[3 * (l * PACK_STEPS + i) + n])
                for n, (src, dst) in enumerate(trio)])
            for copy in loads[-1]:
                copy.start()

    def own(k):
        dense_send(dense_own(x, k), dense_rows(stage, x, c, k), 0, k, to_y).start()
        dense_send(dense_own(1 - x, k), dense_rows(stage, 1 - x, c, k), 1, k, to_z).start()

    loop(DENSE_CHUNKS, own)

    def own_direct(k):
        dense_send(dense_own(1 - x, k), dense_rows(stage, 1 - x, c, k), 4, k, to_y).start()
        dense_send(dense_own(x, k), dense_rows(stage, x, c, k), 5, k, to_z).start()

    loop(DIRECT, own_direct)

    def down_send(p, l):
        rows = pl.ds(p * PIECE, PIECE)
        return remote(down.at[l, rows], w2buf.at[stage * LAYERS + l],
                      ws.at[p, l], wr.at[stage, l], (expert, p))

    def down_arrival(s, l):
        return remote(w2buf.at[s * LAYERS + l], w2buf.at[s * LAYERS + l],
                      ws.at[0, l], wr.at[s, l], to_p)

    def abroad(index):
        return jnp.logical_or(stage != expert, index != expert)

    for l in range(LAYERS):
        for p in range(PIECES):
            @pl.when(abroad(p))
            def _():
                down_send(p, l).start()

    def cut_out(l, i, p, r):
        at = pl.ds(i * PACK_ROWS, PACK_ROWS)
        return pltpu.make_async_copy(cut.at[l, p, at], parts[l][r].at[at], outs.at[l, i, p])

    piece = [lax.rem(ids[h], PIECES) for h in range(HOT)]

    def pick(h, units):
        best = units[0]
        for p in range(1, PIECES):
            best = jnp.where(piece[h] == p, units[p], best)
        return best

    for l in range(LAYERS):
        for i in range(PACK_STEPS):
            for copy in loads[l * PACK_STEPS + i]:
                copy.wait()

            def rows13(j):
                start = pl.multiple_of(i * PACK_ROWS + j * SUB_ROWS, SUB_ROWS)
                at = pl.ds(start, SUB_ROWS)
                units = []
                for p in range(PIECES):
                    lo, hi = p * PIECE, (p + 1) * PIECE
                    units.append(jnp.concatenate([gin[l, at, lo:hi], uin[l, at, lo:hi]], axis=-1))
                    cut[l, p, at, :] = units[p]
                for h in range(HOT):
                    unit = pick(h, units)
                    for b in range(3):
                        hot[l, h, pl.ds(b * HIDDEN + start, SUB_ROWS), :] = unit[:, b * LANES:(b + 1) * LANES]

            loop(PACK_ROWS // SUB_ROWS, rows13)
            for b in range(i * PACK_ROWS // LANES, (i + 1) * PACK_ROWS // LANES):
                def rows2(j, b=b):
                    start = pl.multiple_of(j * SUB_ROWS, SUB_ROWS)
                    units = [din[l, pl.ds(p * PIECE + start, SUB_ROWS), b * LANES:(b + 1) * LANES]
                             for p in range(PIECES)]
                    for h in range(HOT):
                        hot[l, h, pl.ds(HOT13 + b * PIECE + start, SUB_ROWS), :] = pick(h, units)

                loop(PIECE // SUB_ROWS, rows2)
            for here in range(STAGES):
                @pl.when(stage == here)
                def _():
                    for p in range(PIECES):
                        cut_out(l, i, p, (p - here) % PIECES).start()

    swap = [remote(hot.at[1 - c, h], pbuf.at[h], es.at[h], er.at[h], to_p) for h in range(HOT)]
    for h in range(HOT):
        swap[h].start()

    def choose(h, here, other):
        def rows(i):
            at = pl.ds(pl.multiple_of(i * 512, 512), 512)
            hot[c, h, at, :] = jnp.where(here, hot[c, h, at, :], other[h, at, :])

        loop(HOT_ROWS // 512, rows)

    cross = [remote(hot.at[c, h], xbuf.at[h], es.at[2 + h], er.at[2 + h], to_x) for h in range(HOT)]
    for h in range(HOT):
        swap[h].wait_recv()
        choose(h, lax.shift_right_logical(ids[h], 2) == expert, pbuf)
        cross[h].start()

    def relay(k, over_x):
        dense_arrival(0, k).wait_recv()
        dense_on(0, 3, k, to_z).start()
        if over_x:
            dense_on(0, 4, k, to_x).start()
        dense_on(0, 6, k, to_p).start()
        dense_arrival(1, k).wait_recv()
        dense_on(1, 2, k, to_y).start()
        if over_x:
            dense_on(1, 5, k, to_x).start()
        dense_on(1, 7, k, to_p).start()

    loop(DIRECT, lambda k: relay(k, False))
    half_way = DENSE_CHUNKS // 2
    loop(half_way - DIRECT, lambda k: relay(k + DIRECT, True))

    for h in range(HOT):
        cross[h].wait()
        choose(h, lax.shift_right_logical(ids[h], 3) == x, xbuf)
    keep = [pltpu.make_async_copy(hot.at[c, h], hotf.at[stage, h, c], ls.at[h]) for h in range(HOT)]
    give = [remote(hot.at[c, h], hotf.at[stage, h, c], es.at[4 + h], er.at[4 + h], to_p) for h in range(HOT)]
    for h in range(HOT):
        keep[h].start()
        give[h].start()

    def hot_own(k):
        at = pl.ds(pl.multiple_of(k * HOT_CHUNK, HOT_CHUNK), HOT_CHUNK)
        hot_send(hot.at[c, x, at], hot_rows(stage, x, c, k), 0, k, to_y).start()
        hot_send(hot.at[c, 1 - x, at], hot_rows(stage, 1 - x, c, k), 1, k, to_z).start()

    loop(HOT_CHUNKS, hot_own)
    loop(DENSE_CHUNKS - half_way, lambda k: relay(k + half_way, True))

    def hot_relay(k):
        hot_arrival(0, k).wait_recv()
        hot_on(0, 3, k, to_z).start()
        hot_on(0, 4, k, to_x).start()
        hot_on(0, 6, k, to_p).start()
        hot_arrival(1, k).wait_recv()
        hot_on(1, 2, k, to_y).start()
        hot_on(1, 5, k, to_x).start()
        hot_on(1, 7, k, to_p).start()

    loop(HOT_CHUNKS, hot_relay)

    def dense_last(k):
        for i in (4, 5, 2, 3):
            dense_arrival(i, k).wait_recv()
            dense_on(i, 6 + i, k, to_p).start()

    loop(DENSE_CHUNKS, dense_last)

    def hot_last(k):
        for i in (4, 5, 2, 3):
            hot_arrival(i, k).wait_recv()
            hot_on(i, 6 + i, k, to_p).start()

    loop(HOT_CHUNKS, hot_last)

    def dense_end(k):
        for i in range(12):
            if i >= 6:
                dense_arrival(i, k).wait_recv()
            dense_arrival(i, k).wait_send()

    def hot_end(k):
        for i in range(12):
            if i >= 6:
                hot_arrival(i, k).wait_recv()
            hot_arrival(i, k).wait_send()

    loop(DENSE_CHUNKS, dense_end)
    loop(HOT_CHUNKS, hot_end)
    for h in range(HOT):
        swap[h].wait_send()
        keep[h].wait()
        give[h].wait()
    for l in range(LAYERS):
        for p in range(PIECES):
            for i in range(PACK_STEPS):
                cut_out(l, i, p, 0).wait()

            @pl.when(abroad(p))
            def _():
                down_send(p, l).wait_send()

            @pl.when(abroad(p))
            def _():
                down_arrival(p, l).wait_recv()


def spread(dense, gate, up, down, hot_ids):
    sem = pltpu.SemaphoreType.DMA
    total = STAGES * LAYERS
    return pl.pallas_call(
        spread_kernel,
        out_shape=[
            jax.ShapeDtypeStruct((STAGES * 4096, DENSE), BF16),
            jax.ShapeDtypeStruct((STAGES, HOT, LAYERS, HOT_ROWS, LANES), BF16),
            jax.ShapeDtypeStruct((total, PIECE, HIDDEN), BF16),
        ] + [jax.ShapeDtypeStruct((HIDDEN, 2 * PIECE), BF16)] * (LAYERS * PIECES),
        in_specs=[ANY] * 4 + [SMEM],
        out_specs=[ANY] * (3 + LAYERS * PIECES),
        scratch_shapes=[
            pltpu.VMEM((LAYERS, HIDDEN, WIDTH), BF16), pltpu.VMEM((LAYERS, HIDDEN, WIDTH), BF16),
            pltpu.VMEM((LAYERS, WIDTH, HIDDEN), BF16),
            pltpu.VMEM((LAYERS, PIECES, HIDDEN, 2 * PIECE), BF16),
            pltpu.VMEM((LAYERS, HOT, HOT_ROWS, LANES), BF16),
            pltpu.VMEM((HOT, HOT_ROWS, LANES), BF16), pltpu.VMEM((HOT, HOT_ROWS, LANES), BF16),
            sem((12, DENSE_CHUNKS)), sem((12, DENSE_CHUNKS)),
            sem((12, HOT_CHUNKS)), sem((12, HOT_CHUNKS)),
            sem((6,)), sem((6,)), sem((2,)),
            sem((3 * LAYERS * PACK_STEPS,)), sem((LAYERS, PACK_STEPS, PIECES)),
            sem((PIECES, LAYERS)), sem((STAGES, LAYERS)),
        ],
        compiler_params=pltpu.CompilerParams(has_side_effects=True, vmem_limit_bytes=58 << 20),
        cost_estimate=pl.CostEstimate(flops=1 << 32, bytes_accessed=256 << 20, transcendentals=0),
        name="spread",
    )(dense, gate, up, down, hot_ids)


COPY_ROWS = 256
COPY_SLOTS = 12


def dense_copy_kernel(pos, dense, full, out, buf, rs, ws):
    count = STAGES * 4096 // COPY_ROWS
    per_stage = 4096 // COPY_ROWS
    stage = pos[0]

    def rows(k):
        return pl.ds(pl.multiple_of(k * COPY_ROWS, COPY_ROWS), COPY_ROWS)

    def read(k, ref, at):
        slot = lax.rem(k, COPY_SLOTS)
        return pltpu.make_async_copy(ref.at[rows(at)], buf.at[slot], rs.at[slot])

    def write(k):
        slot = lax.rem(k, COPY_SLOTS)
        return pltpu.make_async_copy(buf.at[slot], out.at[rows(k)], ws.at[slot])

    def start(k):
        mine = k // per_stage == stage

        @pl.when(mine)
        def _():
            read(k, dense, k - stage * per_stage).start()

        @pl.when(jnp.logical_not(mine))
        def _():
            read(k, full, k).start()

    ahead = COPY_SLOTS // 2
    loop(ahead, start)

    def step(k):
        @pl.when(k + ahead < count)
        def _():
            @pl.when(k + ahead >= COPY_SLOTS)
            def _():
                write(k + ahead - COPY_SLOTS).wait()

            start(k + ahead)

        read(k, full, k).wait()
        write(k).start()

    loop(count, step)
    loop(COPY_SLOTS, lambda k: write(count - COPY_SLOTS + k).wait())


def dense_copy(stage, dense, full):
    return pl.pallas_call(
        dense_copy_kernel,
        out_shape=jax.ShapeDtypeStruct((STAGES * 4096, DENSE), BF16),
        in_specs=[SMEM, ANY, ANY],
        out_specs=ANY,
        scratch_shapes=[
            pltpu.VMEM((COPY_SLOTS, COPY_ROWS, DENSE), BF16),
            pltpu.SemaphoreType.DMA((COPY_SLOTS,)), pltpu.SemaphoreType.DMA((COPY_SLOTS,)),
        ],
        compiler_params=pltpu.CompilerParams(vmem_limit_bytes=48 << 20),
        cost_estimate=pl.CostEstimate(flops=1 << 28, bytes_accessed=256 << 20, transcendentals=0),
        name="dense_copy",
    )(stage, dense, full)


def spare_kernel(slot, hotf, out13, out2, b13, b2, rs, ws):
    pick = slot[0]
    total = STAGES * LAYERS

    def reads(n, h):
        src = hotf.at[n // LAYERS, h, n % LAYERS]
        for b in range(3):
            yield pltpu.make_async_copy(
                src.at[pl.ds(b * HIDDEN, HIDDEN)], b13.at[n, :, pl.ds(b * LANES, LANES)], rs.at[n])
        for b in range(16):
            yield pltpu.make_async_copy(
                src.at[pl.ds(HOT13 + b * PIECE, PIECE)], b2.at[n, :, pl.ds(b * LANES, LANES)], rs.at[n])

    @pl.when(pick >= 0)
    def _():
        for n in range(total):
            for copy in reads(n, jnp.maximum(pick, 0)):
                copy.start()

    @pl.when(pick < 0)
    def _():
        for n in range(total):
            b13[n] = jnp.zeros((HIDDEN, 2 * PIECE), BF16)
            b2[n] = jnp.zeros((PIECE, HIDDEN), BF16)

    writes = []
    for n in range(total):
        @pl.when(pick >= 0)
        def _():
            pltpu.make_async_copy(out13.at[n], b13.at[n], rs.at[n]).wait()
            pltpu.make_async_copy(out2.at[n], b2.at[n], rs.at[n]).wait()

        writes.append(pltpu.make_async_copy(b13.at[n], out13.at[n], ws.at[n]))
        writes.append(pltpu.make_async_copy(b2.at[n], out2.at[n], ws.at[total + n]))
        writes[-2].start()
        writes[-1].start()
    for copy in writes:
        copy.wait()


def spare(slot, hotf):
    total = STAGES * LAYERS
    return pl.pallas_call(
        spare_kernel,
        out_shape=[
            jax.ShapeDtypeStruct((total, HIDDEN, 2 * PIECE), BF16),
            jax.ShapeDtypeStruct((total, PIECE, HIDDEN), BF16),
        ],
        in_specs=[SMEM, ANY],
        out_specs=[ANY, ANY],
        scratch_shapes=[
            pltpu.VMEM((total, HIDDEN, 2 * PIECE), BF16),
            pltpu.VMEM((total, PIECE, HIDDEN), BF16),
            pltpu.SemaphoreType.DMA((total,)), pltpu.SemaphoreType.DMA((2 * total,)),
        ],
        compiler_params=pltpu.CompilerParams(vmem_limit_bytes=48 << 20),
        cost_estimate=pl.CostEstimate(flops=1 << 26, bytes_accessed=36 << 20, transcendentals=0),
        name="spare",
    )(slot, hotf)


def place2_kernel(pos, down, w2buf, out, buf, rs, ws):
    stage, column = pos[0], pos[1]
    total = STAGES * LAYERS
    own = pl.ds(pl.multiple_of(column * PIECE, PIECE), PIECE)
    for n in range(total):
        mine = jnp.logical_and(stage == column, stage == n // LAYERS)

        @pl.when(mine)
        def _():
            pltpu.make_async_copy(down.at[n % LAYERS, own], buf.at[n], rs.at[n]).start()

        @pl.when(jnp.logical_not(mine))
        def _():
            pltpu.make_async_copy(w2buf.at[n], buf.at[n], rs.at[n]).start()

    writes = [pltpu.make_async_copy(buf.at[n], out.at[n], ws.at[n]) for n in range(total)]
    for n in range(total):
        pltpu.make_async_copy(w2buf.at[n], buf.at[n], rs.at[n]).wait()
        writes[n].start()
    for write in writes:
        write.wait()


def place2(pos, down, w2buf):
    total = STAGES * LAYERS
    return pl.pallas_call(
        place2_kernel,
        out_shape=jax.ShapeDtypeStruct((total, PIECE, HIDDEN), BF16),
        in_specs=[SMEM, ANY, ANY],
        out_specs=ANY,
        scratch_shapes=[
            pltpu.VMEM((total, PIECE, HIDDEN), BF16),
            pltpu.SemaphoreType.DMA((total,)), pltpu.SemaphoreType.DMA((total,)),
        ],
        compiler_params=pltpu.CompilerParams(vmem_limit_bytes=48 << 20),
        cost_estimate=pl.CostEstimate(flops=1 << 25, bytes_accessed=12 << 20, transcendentals=0),
        name="place2",
    )(pos, down, w2buf)


def place13_kernel(layer, pos, *refs):
    moved, own, (out, buf, rs, ws) = refs[:4], refs[4], refs[-4:]
    stage, column = pos[0], pos[1]
    for r in range(PIECES):
        if r == 0:
            @pl.when(stage == column)
            def _():
                pltpu.make_async_copy(own, buf.at[0], rs.at[0]).start()

            @pl.when(stage != column)
            def _():
                pltpu.make_async_copy(moved[0], buf.at[0], rs.at[0]).start()
        else:
            pltpu.make_async_copy(moved[r], buf.at[r], rs.at[r]).start()
    writes = []
    for r in range(PIECES):
        n = lax.rem(column - r + PIECES, PIECES) * LAYERS + layer
        writes.append(pltpu.make_async_copy(buf.at[r], out.at[n], ws.at[r]))
    for r in range(PIECES):
        pltpu.make_async_copy(moved[r], buf.at[r], rs.at[r]).wait()
        writes[r].start()
    for write in writes:
        write.wait()


def place13(layer, pos, moved, own, out=None):
    operands = [pos, *moved, own] + ([] if out is None else [out])
    return pl.pallas_call(
        functools.partial(place13_kernel, layer),
        out_shape=jax.ShapeDtypeStruct((STAGES * LAYERS, HIDDEN, 2 * PIECE), BF16),
        in_specs=[SMEM] + [ANY] * (len(operands) - 1),
        out_specs=ANY,
        scratch_shapes=[
            pltpu.VMEM((PIECES, HIDDEN, 2 * PIECE), BF16),
            pltpu.SemaphoreType.DMA((PIECES,)), pltpu.SemaphoreType.DMA((PIECES,)),
        ],
        input_output_aliases={} if out is None else {len(operands) - 1: 0},
        compiler_params=pltpu.CompilerParams(vmem_limit_bytes=48 << 20),
        cost_estimate=pl.CostEstimate(flops=1 << 25, bytes_accessed=12 << 20, transcendentals=0),
        name=f"place13_{layer}",
    )(*operands)


def solution(mesh):
    flat_axes = ('stage', 'expert')

    def pairs(r):
        every = [(s * 4 + e, e * 4 + (s + r) % 4) for s in range(4) for e in range(4)]
        return [pair for pair in every if pair[0] != pair[1]]

    def local_move(w_gate, w_up, w_down, dense, hot_ids, spare_map):
        stage = lax.axis_index('stage').astype(jnp.int32)[None]
        column = lax.axis_index('expert').astype(jnp.int32)[None]
        pos = jnp.concatenate([stage, column])
        dense, w_down = dense.reshape(4096, DENSE), w_down[:, 0]
        full, hotf, w2buf, *parts = spread(dense, w_gate[:, 0], w_up[:, 0], w_down, hot_ids)
        moved = [lax.ppermute(part, flat_axes, pairs(i % 4)) for i, part in enumerate(parts)]
        dense_out = dense_copy(stage, dense, full).reshape(STAGES * LAYERS, HIDDEN, DENSE)
        spare13, spare2 = spare(spare_map, hotf)
        w2 = place2(pos, w_down, w2buf)
        w13 = place13(0, pos, moved[:4], parts[0])
        w13 = place13(1, pos, moved[4:], parts[4], w13)
        return w13[:, None], w2[:, None], dense_out, spare13[:, None], spare2[:, None]

    expert_spec = P('stage', 'expert', None, None)
    unit_spec = P(None, flat_axes, None, None)
    return jax.shard_map(
        local_move,
        mesh=mesh,
        in_specs=(expert_spec, expert_spec, expert_spec, P('stage', None, None), P(None), P(flat_axes)),
        out_specs=(unit_spec, unit_spec, P(None, None, None), unit_spec, unit_spec),
        check_vma=False,
    )
```

```python
import functools

import jax
import jax.numpy as jnp
from jax import lax
from jax.experimental import pallas as pl
from jax.experimental.pallas import tpu as pltpu
from jax.sharding import PartitionSpec as P


MESH = pl.DeviceIdType.MESH
ANY = pl.BlockSpec(memory_space=pl.ANY)
SMEM = pl.BlockSpec(memory_space=pltpu.SMEM)
BF16 = jnp.bfloat16

LAYERS, HIDDEN, WIDTH, DENSE = 2, 2048, 768, 4096
PIECES, PIECE = 4, 192
STAGES = 4
HOT = 2
LANES = 128
HOT13 = 3 * HIDDEN
HOT_ROWS = HOT13 + 16 * PIECE
DENSE_CHUNKS = 16
DENSE_CHUNK = 1024 // DENSE_CHUNKS
HOT_CHUNKS = 1
HOT_CHUNK = HOT_ROWS // HOT_CHUNKS
PACK_STEPS = 4
PACK_ROWS = HIDDEN // PACK_STEPS
SUB_ROWS = 64


def loop(count, body):
    def step(k, carry):
        body(k)
        return carry

    lax.fori_loop(0, count, step, 0)


def spread_kernel(first, dense, gate, up, down, ids, full, hotf, w2buf, *refs):
    parts, refs = [refs[:4], refs[4:8]], refs[8:]
    gin, uin, din, cut, hot, pbuf, ours, xbuf = refs[:8]
    ds, dr, hs, hr, es, er, ls, ins, outs, ws, wr = refs[8:]
    stage, expert = lax.axis_index('stage'), lax.axis_index('expert')
    z, y = stage // 2, stage % 2
    x, c = expert // 2, expert % 2
    to_y = (z * 2 + 1 - y, expert)
    to_z = ((1 - z) * 2 + y, expert)
    to_x = (stage, (1 - x) * 2 + c)
    to_p = (stage, x * 2 + 1 - c)
    at_y, at_z, at_yz = z * 2 + 1 - y, (1 - z) * 2 + y, (1 - z) * 2 + 1 - y
    flows = [(at_y, x), (at_z, 1 - x), (at_yz, 1 - x), (at_yz, x), (at_y, 1 - x), (at_z, x)]

    def remote(src, dst, send, recv, to):
        return pltpu.make_async_remote_copy(
            src_ref=src, dst_ref=dst, send_sem=send, recv_sem=recv, device_id=to, device_id_type=MESH)

    def dense_rows(st, half, core, k):
        start = st * 4096 + half * 2048 + core * 1024 + k * DENSE_CHUNK
        return full.at[pl.ds(pl.multiple_of(start, DENSE_CHUNK), DENSE_CHUNK)]

    def hot_rows(st, half, core, k):
        return hotf.at[st, half, core, pl.ds(pl.multiple_of(k * HOT_CHUNK, HOT_CHUNK), HOT_CHUNK)]

    def dense_send(src, dst, flow, k, to):
        return remote(src, dst, ds.at[flow, k], dr.at[flow, k], to)

    def hot_send(src, dst, flow, k, to):
        return remote(src, dst, hs.at[flow, k], hr.at[flow, k], to)

    def dense_own(half, k):
        start = half * 2048 + c * 1024 + k * DENSE_CHUNK
        return dense.at[pl.ds(pl.multiple_of(start, DENSE_CHUNK), DENSE_CHUNK)]

    def dense_on(i, flow, k, to):
        ref = dense_rows(*flows[i], c, k)
        return dense_send(ref, ref, flow, k, to)

    def hot_on(i, flow, k, to):
        ref = hot_rows(*flows[i], c, k)
        return hot_send(ref, ref, flow, k, to)

    def dense_arrival(flow, k):
        ref = dense_rows(*flows[flow % 6], c if flow < 6 else 1 - c, k)
        return dense_send(ref, ref, flow, k, to_p)

    def hot_arrival(flow, k):
        ref = hot_rows(*flows[flow % 6], c if flow < 6 else 1 - c, k)
        return hot_send(ref, ref, flow, k, to_p)

    loads = []
    for l in range(LAYERS):
        for i in range(PACK_STEPS):
            at = pl.ds(i * PACK_ROWS, PACK_ROWS)
            trio = ((gate.at[l, at], gin.at[l, at]), (up.at[l, at], uin.at[l, at]),
                    (down.at[l, :, at], din.at[l, :, at]))
            loads.append([
                pltpu.make_async_copy(src, dst, ins.at[3 * (l * PACK_STEPS + i) + n])
                for n, (src, dst) in enumerate(trio)])
            for copy in loads[-1]:
                copy.start()

    def own(k):
        dense_send(dense_own(x, k), dense_rows(stage, x, c, k), 0, k, to_y).start()
        dense_send(dense_own(1 - x, k), dense_rows(stage, 1 - x, c, k), 1, k, to_z).start()

    loop(DENSE_CHUNKS, own)

    least = 3 if first is None else 1
    most = least if first is None else least + 1
    skips4 = least if first is None else least + c
    skips5 = least if first is None else most - c

    def direct4(k):
        dense_send(dense_own(1 - x, k), dense_rows(stage, 1 - x, c, k), 4, k, to_y).start()

    def direct5(k):
        dense_send(dense_own(x, k), dense_rows(stage, x, c, k), 5, k, to_z).start()

    for k in range(most):
        if k < least:
            direct4(k)
            direct5(k)
        else:
            pl.when(k < skips4)(functools.partial(direct4, k))
            pl.when(k < skips5)(functools.partial(direct5, k))

    def down_send(p, l):
        rows = pl.ds(p * PIECE, PIECE)
        return remote(down.at[l, rows], w2buf.at[stage * LAYERS + l],
                      ws.at[p, l], wr.at[stage, l], (expert, p))

    def down_arrival(s, l):
        return remote(w2buf.at[s * LAYERS + l], w2buf.at[s * LAYERS + l],
                      ws.at[0, l], wr.at[s, l], to_p)

    def abroad(index):
        return jnp.logical_or(stage != expert, index != expert)

    for l in (0,):
        for p in range(PIECES):
            @pl.when(abroad(p))
            def _():
                down_send(p, l).start()

    def cut_out(l, i, p, r):
        at = pl.ds(i * PACK_ROWS, PACK_ROWS)
        return pltpu.make_async_copy(cut.at[l, p, at], parts[l][r].at[at], outs.at[l, i, p])

    piece = [lax.rem(ids[h], PIECES) for h in range(HOT)]

    def pick(h, units):
        best = units[0]
        for p in range(1, PIECES):
            best = jnp.where(piece[h] == p, units[p], best)
        return best

    for l in range(LAYERS):
        for i in range(PACK_STEPS):
            for copy in loads[l * PACK_STEPS + i]:
                copy.wait()

            def rows13(j):
                start = pl.multiple_of(i * PACK_ROWS + j * SUB_ROWS, SUB_ROWS)
                at = pl.ds(start, SUB_ROWS)
                units = []
                for p in range(PIECES):
                    lo, hi = p * PIECE, (p + 1) * PIECE
                    units.append(jnp.concatenate([gin[l, at, lo:hi], uin[l, at, lo:hi]], axis=-1))
                    cut[l, p, at, :] = units[p]
                for h in range(HOT):
                    unit = pick(h, units)
                    for b in range(3):
                        hot[l, h, pl.ds(b * HIDDEN + start, SUB_ROWS), :] = unit[:, b * LANES:(b + 1) * LANES]

            loop(PACK_ROWS // SUB_ROWS, rows13)
            for b in range(i * PACK_ROWS // LANES, (i + 1) * PACK_ROWS // LANES):
                def rows2(j, b=b):
                    start = pl.multiple_of(j * SUB_ROWS, SUB_ROWS)
                    units = [din[l, pl.ds(p * PIECE + start, SUB_ROWS), b * LANES:(b + 1) * LANES]
                             for p in range(PIECES)]
                    for h in range(HOT):
                        hot[l, h, pl.ds(HOT13 + b * PIECE + start, SUB_ROWS), :] = pick(h, units)

                loop(PIECE // SUB_ROWS, rows2)
            for here in range(STAGES):
                @pl.when(stage == here)
                def _():
                    for p in range(PIECES):
                        cut_out(l, i, p, (p - here) % PIECES).start()

    held = range(HOT) if first is None else ((x + first) % 2,)
    swap = [remote(hot.at[1 - c, h], pbuf.at[h], es.at[n], er.at[n], to_p) for n, h in enumerate(held)]
    for copy in swap:
        copy.start()

    def choose(h, here, mine, other):
        def rows(i):
            at = pl.ds(pl.multiple_of(i * 512, 512), 512)
            ours[h, at, :] = jnp.where(here, mine[h, at, :], other[h, at, :])

        loop(HOT_ROWS // 512, rows)

    landing = xbuf if first is None else ours
    cross = [remote(ours.at[h], landing.at[h], es.at[2 + n], er.at[2 + n], to_x) for n, h in enumerate(held)]
    for n, h in enumerate(held):
        swap[n].wait_recv()
        choose(h, lax.shift_right_logical(ids[h], 2) == expert, hot.at[c], pbuf)
        cross[n].start()

    def relay(k, over4, over5):
        dense_arrival(0, k).wait_recv()
        dense_on(0, 3, k, to_z).start()
        pl.when(over4)(lambda: dense_on(0, 4, k, to_x).start())
        dense_on(0, 6, k, to_p).start()
        dense_arrival(1, k).wait_recv()
        dense_on(1, 2, k, to_y).start()
        pl.when(over5)(lambda: dense_on(1, 5, k, to_x).start())
        dense_on(1, 7, k, to_p).start()

    for k in range(most):
        relay(k, k >= skips4, k >= skips5)
    half_way = DENSE_CHUNKS // 2
    loop(half_way - most, lambda k: relay(k + most, True, True))

    for n, h in enumerate(held):
        cross[n].wait()
        if first is None:
            choose(h, lax.shift_right_logical(ids[h], 3) == x, ours, xbuf)
    keep = [pltpu.make_async_copy(ours.at[h], hotf.at[stage, h, c], ls.at[h]) for h in range(HOT)]
    give = [remote(ours.at[h], hotf.at[stage, h, c], es.at[4 + h], er.at[4 + h], to_p) for h in range(HOT)]
    for h in range(HOT):
        keep[h].start()
        give[h].start()

    def hot_own(k):
        at = pl.ds(pl.multiple_of(k * HOT_CHUNK, HOT_CHUNK), HOT_CHUNK)
        hot_send(ours.at[x, at], hot_rows(stage, x, c, k), 0, k, to_y).start()
        hot_send(ours.at[1 - x, at], hot_rows(stage, 1 - x, c, k), 1, k, to_z).start()

    loop(HOT_CHUNKS, hot_own)
    loop(DENSE_CHUNKS - half_way, lambda k: relay(k + half_way, True, True))

    def hot_relay(k):
        hot_arrival(0, k).wait_recv()
        hot_on(0, 3, k, to_z).start()
        hot_on(0, 4, k, to_x).start()
        hot_on(0, 6, k, to_p).start()
        hot_arrival(1, k).wait_recv()
        hot_on(1, 2, k, to_y).start()
        hot_on(1, 5, k, to_x).start()
        hot_on(1, 7, k, to_p).start()

    loop(HOT_CHUNKS, hot_relay)

    for l in (1,):
        for p in range(PIECES):
            @pl.when(abroad(p))
            def _():
                down_send(p, l).start()

    def dense_last(k):
        for i in (4, 5, 2, 3):
            dense_arrival(i, k).wait_recv()
            dense_on(i, 6 + i, k, to_p).start()

    loop(DENSE_CHUNKS, dense_last)

    def hot_last(k):
        for i in (4, 5, 2, 3):
            hot_arrival(i, k).wait_recv()
            hot_on(i, 6 + i, k, to_p).start()

    loop(HOT_CHUNKS, hot_last)

    def dense_end(k):
        for i in range(12):
            if i >= 6:
                dense_arrival(i, k).wait_recv()
            dense_arrival(i, k).wait_send()

    def hot_end(k):
        for i in range(12):
            if i >= 6:
                hot_arrival(i, k).wait_recv()
            hot_arrival(i, k).wait_send()

    loop(DENSE_CHUNKS, dense_end)
    loop(HOT_CHUNKS, hot_end)
    for copy in swap:
        copy.wait_send()
    for h in range(HOT):
        keep[h].wait()
        give[h].wait()
    for l in range(LAYERS):
        for p in range(PIECES):
            for i in range(PACK_STEPS):
                cut_out(l, i, p, 0).wait()

            @pl.when(abroad(p))
            def _():
                down_send(p, l).wait_send()

            @pl.when(abroad(p))
            def _():
                down_arrival(p, l).wait_recv()


def spread(first, dense, gate, up, down, hot_ids):
    sem = pltpu.SemaphoreType.DMA
    total = STAGES * LAYERS
    return pl.pallas_call(
        functools.partial(spread_kernel, first),
        out_shape=[
            jax.ShapeDtypeStruct((STAGES * 4096, DENSE), BF16),
            jax.ShapeDtypeStruct((STAGES, HOT, LAYERS, HOT_ROWS, LANES), BF16),
            jax.ShapeDtypeStruct((total, PIECE, HIDDEN), BF16),
        ] + [jax.ShapeDtypeStruct((HIDDEN, 2 * PIECE), BF16)] * (LAYERS * PIECES),
        in_specs=[ANY] * 4 + [SMEM],
        out_specs=[ANY] * (3 + LAYERS * PIECES),
        scratch_shapes=[
            pltpu.VMEM((LAYERS, HIDDEN, WIDTH), BF16), pltpu.VMEM((LAYERS, HIDDEN, WIDTH), BF16),
            pltpu.VMEM((LAYERS, WIDTH, HIDDEN), BF16),
            pltpu.VMEM((LAYERS, PIECES, HIDDEN, 2 * PIECE), BF16),
            pltpu.VMEM((LAYERS, HOT, HOT_ROWS, LANES), BF16),
            pltpu.VMEM((HOT, HOT_ROWS, LANES), BF16), pltpu.VMEM((HOT, HOT_ROWS, LANES), BF16),
            pltpu.VMEM((HOT, HOT_ROWS, LANES), BF16),
            sem((12, DENSE_CHUNKS)), sem((12, DENSE_CHUNKS)),
            sem((12, HOT_CHUNKS)), sem((12, HOT_CHUNKS)),
            sem((6,)), sem((6,)), sem((2,)),
            sem((3 * LAYERS * PACK_STEPS,)), sem((LAYERS, PACK_STEPS, PIECES)),
            sem((PIECES, LAYERS)), sem((STAGES, LAYERS)),
        ],
        compiler_params=pltpu.CompilerParams(has_side_effects=True, vmem_limit_bytes=58 << 20),
        cost_estimate=pl.CostEstimate(flops=1 << 32, bytes_accessed=256 << 20, transcendentals=0),
        name="spread" if first is None else f"spread_{first}",
    )(dense, gate, up, down, hot_ids)


COPY_ROWS = 256
COPY_SLOTS = 12


def dense_copy_kernel(pos, dense, full, out, buf, rs, ws):
    count = STAGES * 4096 // COPY_ROWS
    per_stage = 4096 // COPY_ROWS
    stage = pos[0]

    def rows(k):
        return pl.ds(pl.multiple_of(k * COPY_ROWS, COPY_ROWS), COPY_ROWS)

    def read(k, ref, at):
        slot = lax.rem(k, COPY_SLOTS)
        return pltpu.make_async_copy(ref.at[rows(at)], buf.at[slot], rs.at[slot])

    def write(k):
        slot = lax.rem(k, COPY_SLOTS)
        return pltpu.make_async_copy(buf.at[slot], out.at[rows(k)], ws.at[slot])

    def start(k):
        mine = k // per_stage == stage

        @pl.when(mine)
        def _():
            read(k, dense, k - stage * per_stage).start()

        @pl.when(jnp.logical_not(mine))
        def _():
            read(k, full, k).start()

    ahead = COPY_SLOTS // 2
    loop(ahead, start)

    def step(k):
        @pl.when(k + ahead < count)
        def _():
            @pl.when(k + ahead >= COPY_SLOTS)
            def _():
                write(k + ahead - COPY_SLOTS).wait()

            start(k + ahead)

        read(k, full, k).wait()
        write(k).start()

    loop(count, step)
    loop(COPY_SLOTS, lambda k: write(count - COPY_SLOTS + k).wait())


def dense_copy(stage, dense, full):
    return pl.pallas_call(
        dense_copy_kernel,
        out_shape=jax.ShapeDtypeStruct((STAGES * 4096, DENSE), BF16),
        in_specs=[SMEM, ANY, ANY],
        out_specs=ANY,
        scratch_shapes=[
            pltpu.VMEM((COPY_SLOTS, COPY_ROWS, DENSE), BF16),
            pltpu.SemaphoreType.DMA((COPY_SLOTS,)), pltpu.SemaphoreType.DMA((COPY_SLOTS,)),
        ],
        compiler_params=pltpu.CompilerParams(vmem_limit_bytes=48 << 20),
        cost_estimate=pl.CostEstimate(flops=1 << 28, bytes_accessed=256 << 20, transcendentals=0),
        name="dense_copy",
    )(stage, dense, full)


def spare_kernel(slot, hotf, out13, out2, b13, b2, rs, ws):
    pick = slot[0]
    total = STAGES * LAYERS

    def reads(n, h):
        src = hotf.at[n // LAYERS, h, n % LAYERS]
        for b in range(3):
            yield pltpu.make_async_copy(
                src.at[pl.ds(b * HIDDEN, HIDDEN)], b13.at[n, :, pl.ds(b * LANES, LANES)], rs.at[n])
        for b in range(16):
            yield pltpu.make_async_copy(
                src.at[pl.ds(HOT13 + b * PIECE, PIECE)], b2.at[n, :, pl.ds(b * LANES, LANES)], rs.at[n])

    @pl.when(pick >= 0)
    def _():
        for n in range(total):
            for copy in reads(n, jnp.maximum(pick, 0)):
                copy.start()

    @pl.when(pick < 0)
    def _():
        for n in range(total):
            b13[n] = jnp.zeros((HIDDEN, 2 * PIECE), BF16)
            b2[n] = jnp.zeros((PIECE, HIDDEN), BF16)

    writes = []
    for n in range(total):
        @pl.when(pick >= 0)
        def _():
            pltpu.make_async_copy(out13.at[n], b13.at[n], rs.at[n]).wait()
            pltpu.make_async_copy(out2.at[n], b2.at[n], rs.at[n]).wait()

        writes.append(pltpu.make_async_copy(b13.at[n], out13.at[n], ws.at[n]))
        writes.append(pltpu.make_async_copy(b2.at[n], out2.at[n], ws.at[total + n]))
        writes[-2].start()
        writes[-1].start()
    for copy in writes:
        copy.wait()


def spare(slot, hotf):
    total = STAGES * LAYERS
    return pl.pallas_call(
        spare_kernel,
        out_shape=[
            jax.ShapeDtypeStruct((total, HIDDEN, 2 * PIECE), BF16),
            jax.ShapeDtypeStruct((total, PIECE, HIDDEN), BF16),
        ],
        in_specs=[SMEM, ANY],
        out_specs=[ANY, ANY],
        scratch_shapes=[
            pltpu.VMEM((total, HIDDEN, 2 * PIECE), BF16),
            pltpu.VMEM((total, PIECE, HIDDEN), BF16),
            pltpu.SemaphoreType.DMA((total,)), pltpu.SemaphoreType.DMA((2 * total,)),
        ],
        compiler_params=pltpu.CompilerParams(vmem_limit_bytes=48 << 20),
        cost_estimate=pl.CostEstimate(flops=1 << 26, bytes_accessed=36 << 20, transcendentals=0),
        name="spare",
    )(slot, hotf)


def place2_kernel(pos, down, w2buf, out, buf, rs, ws):
    stage, column = pos[0], pos[1]
    total = STAGES * LAYERS
    own = pl.ds(pl.multiple_of(column * PIECE, PIECE), PIECE)
    for n in range(total):
        mine = jnp.logical_and(stage == column, stage == n // LAYERS)

        @pl.when(mine)
        def _():
            pltpu.make_async_copy(down.at[n % LAYERS, own], buf.at[n], rs.at[n]).start()

        @pl.when(jnp.logical_not(mine))
        def _():
            pltpu.make_async_copy(w2buf.at[n], buf.at[n], rs.at[n]).start()

    writes = [pltpu.make_async_copy(buf.at[n], out.at[n], ws.at[n]) for n in range(total)]
    for n in range(total):
        pltpu.make_async_copy(w2buf.at[n], buf.at[n], rs.at[n]).wait()
        writes[n].start()
    for write in writes:
        write.wait()


def place2(pos, down, w2buf):
    total = STAGES * LAYERS
    return pl.pallas_call(
        place2_kernel,
        out_shape=jax.ShapeDtypeStruct((total, PIECE, HIDDEN), BF16),
        in_specs=[SMEM, ANY, ANY],
        out_specs=ANY,
        scratch_shapes=[
            pltpu.VMEM((total, PIECE, HIDDEN), BF16),
            pltpu.SemaphoreType.DMA((total,)), pltpu.SemaphoreType.DMA((total,)),
        ],
        compiler_params=pltpu.CompilerParams(vmem_limit_bytes=48 << 20),
        cost_estimate=pl.CostEstimate(flops=1 << 25, bytes_accessed=12 << 20, transcendentals=0),
        name="place2",
    )(pos, down, w2buf)


def place13_kernel(layer, pos, *refs):
    moved, own, (out, buf, rs, ws) = refs[:4], refs[4], refs[-4:]
    stage, column = pos[0], pos[1]
    for r in range(PIECES):
        if r == 0:
            @pl.when(stage == column)
            def _():
                pltpu.make_async_copy(own, buf.at[0], rs.at[0]).start()

            @pl.when(stage != column)
            def _():
                pltpu.make_async_copy(moved[0], buf.at[0], rs.at[0]).start()
        else:
            pltpu.make_async_copy(moved[r], buf.at[r], rs.at[r]).start()
    writes = []
    for r in range(PIECES):
        n = lax.rem(column - r + PIECES, PIECES) * LAYERS + layer
        writes.append(pltpu.make_async_copy(buf.at[r], out.at[n], ws.at[r]))
    for r in range(PIECES):
        pltpu.make_async_copy(moved[r], buf.at[r], rs.at[r]).wait()
        writes[r].start()
    for write in writes:
        write.wait()


def place13(layer, pos, moved, own, out=None):
    operands = [pos, *moved, own] + ([] if out is None else [out])
    return pl.pallas_call(
        functools.partial(place13_kernel, layer),
        out_shape=jax.ShapeDtypeStruct((STAGES * LAYERS, HIDDEN, 2 * PIECE), BF16),
        in_specs=[SMEM] + [ANY] * (len(operands) - 1),
        out_specs=ANY,
        scratch_shapes=[
            pltpu.VMEM((PIECES, HIDDEN, 2 * PIECE), BF16),
            pltpu.SemaphoreType.DMA((PIECES,)), pltpu.SemaphoreType.DMA((PIECES,)),
        ],
        input_output_aliases={} if out is None else {len(operands) - 1: 0},
        compiler_params=pltpu.CompilerParams(vmem_limit_bytes=48 << 20),
        cost_estimate=pl.CostEstimate(flops=1 << 25, bytes_accessed=12 << 20, transcendentals=0),
        name=f"place13_{layer}",
    )(*operands)


def solution(mesh):
    flat_axes = ('stage', 'expert')

    def pairs(r):
        every = [(s * 4 + e, e * 4 + (s + r) % 4) for s in range(4) for e in range(4)]
        return [pair for pair in every if pair[0] != pair[1]]

    def local_move(w_gate, w_up, w_down, dense, hot_ids, spare_map):
        stage = lax.axis_index('stage').astype(jnp.int32)[None]
        column = lax.axis_index('expert').astype(jnp.int32)[None]
        pos = jnp.concatenate([stage, column])
        dense, w_down = dense.reshape(4096, DENSE), w_down[:, 0]
        holder = lax.shift_right_logical(hot_ids, 3)
        case = jnp.where(holder[0] == holder[1], 0, 1 + holder[0])
        full, hotf, w2buf, *parts = lax.switch(
            case, [functools.partial(spread, first) for first in (None, 0, 1)],
            dense, w_gate[:, 0], w_up[:, 0], w_down, hot_ids)
        moved = [lax.ppermute(part, flat_axes, pairs(i % 4)) for i, part in enumerate(parts)]
        dense_out = dense_copy(stage, dense, full).reshape(STAGES * LAYERS, HIDDEN, DENSE)
        spare13, spare2 = spare(spare_map, hotf)
        w2 = place2(pos, w_down, w2buf)
        w13 = place13(0, pos, moved[:4], parts[0])
        w13 = place13(1, pos, moved[4:], parts[4], w13)
        return w13[:, None], w2[:, None], dense_out, spare13[:, None], spare2[:, None]

    expert_spec = P('stage', 'expert', None, None)
    unit_spec = P(None, flat_axes, None, None)
    return jax.shard_map(
        local_move,
        mesh=mesh,
        in_specs=(expert_spec, expert_spec, expert_spec, P('stage', None, None), P(None), P(flat_axes)),
        out_specs=(unit_spec, unit_spec, P(None, None, None), unit_spec, unit_spec),
        check_vma=False,
    )
```

```python
import functools

import jax
import jax.numpy as jnp
from jax import lax
from jax.experimental import pallas as pl
from jax.experimental.pallas import tpu as pltpu
from jax.sharding import PartitionSpec as P


MESH = pl.DeviceIdType.MESH
ANY = pl.BlockSpec(memory_space=pl.ANY)
SMEM = pl.BlockSpec(memory_space=pltpu.SMEM)
BF16 = jnp.bfloat16

LAYERS, HIDDEN, WIDTH, DENSE = 2, 2048, 768, 4096
PIECES, PIECE = 4, 192
STAGES = 4
HOT = 2
LANES = 128
HOT13 = 3 * HIDDEN
HOT_ROWS = HOT13 + 16 * PIECE
DENSE_CHUNKS = ((0, 128), (128, 128), (256, 256), (512, 256), (768, 256))
HOT_CHUNKS = 1
HOT_CHUNK = HOT_ROWS // HOT_CHUNKS
PACK_STEPS = 4
PACK_ROWS = HIDDEN // PACK_STEPS
SUB_ROWS = 64


def loop(count, body):
    def step(k, carry):
        body(k)
        return carry

    lax.fori_loop(0, count, step, 0)


def spread_kernel(first, dense, gate, up, down, ids, full, hotf, w2buf, *refs):
    parts, refs = [refs[:4], refs[4:8]], refs[8:]
    gin, uin, din, cut, hot, pbuf, ours, xbuf = refs[:8]
    ds, dr, hs, hr, es, er, ls, ins, outs, ws, wr = refs[8:]
    stage, expert = lax.axis_index('stage'), lax.axis_index('expert')
    z, y = stage // 2, stage % 2
    x, c = expert // 2, expert % 2
    to_y = (z * 2 + 1 - y, expert)
    to_z = ((1 - z) * 2 + y, expert)
    to_x = (stage, (1 - x) * 2 + c)
    to_p = (stage, x * 2 + 1 - c)
    at_y, at_z, at_yz = z * 2 + 1 - y, (1 - z) * 2 + y, (1 - z) * 2 + 1 - y
    flows = [(at_y, x), (at_z, 1 - x), (at_yz, 1 - x), (at_yz, x), (at_y, 1 - x), (at_z, x)]

    def remote(src, dst, send, recv, to):
        return pltpu.make_async_remote_copy(
            src_ref=src, dst_ref=dst, send_sem=send, recv_sem=recv, device_id=to, device_id_type=MESH)

    def part_of(k, skip=0):
        start, size = DENSE_CHUNKS[k]
        cut = max(start, min(skip, start + size))
        return cut, start + size - cut

    def dense_rows(st, half, core, part):
        start = st * 4096 + half * 2048 + core * 1024 + part[0]
        return full.at[pl.ds(pl.multiple_of(start, 32), part[1])]

    def hot_rows(st, half, core, k):
        return hotf.at[st, half, core, pl.ds(pl.multiple_of(k * HOT_CHUNK, HOT_CHUNK), HOT_CHUNK)]

    def dense_send(src, dst, flow, k, to):
        return remote(src, dst, ds.at[flow, k], dr.at[flow, k], to)

    def hot_send(src, dst, flow, k, to):
        return remote(src, dst, hs.at[flow, k], hr.at[flow, k], to)

    def dense_own(half, flow, k, part, to):
        start = half * 2048 + c * 1024 + part[0]
        src = dense.at[pl.ds(pl.multiple_of(start, 32), part[1])]
        dense_send(src, dense_rows(stage, half, c, part), flow, k, to).start()

    def dense_on(i, flow, k, to, skip=0):
        part = part_of(k, skip)
        if part[1]:
            ref = dense_rows(*flows[i], c, part)
            dense_send(ref, ref, flow, k, to).start()

    def hot_on(i, flow, k, to):
        ref = hot_rows(*flows[i], c, k)
        return hot_send(ref, ref, flow, k, to)

    def dense_arrival(flow, k):
        ref = dense_rows(*flows[flow % 6], c if flow < 6 else 1 - c, DENSE_CHUNKS[k])
        return dense_send(ref, ref, flow, k, to_p)

    def hot_arrival(flow, k):
        ref = hot_rows(*flows[flow % 6], c if flow < 6 else 1 - c, k)
        return hot_send(ref, ref, flow, k, to_p)

    loads = []
    for l in range(LAYERS):
        for i in range(PACK_STEPS):
            at = pl.ds(i * PACK_ROWS, PACK_ROWS)
            trio = ((gate.at[l, at], gin.at[l, at]), (up.at[l, at], uin.at[l, at]),
                    (down.at[l, :, at], din.at[l, :, at]))
            loads.append([
                pltpu.make_async_copy(src, dst, ins.at[3 * (l * PACK_STEPS + i) + n])
                for n, (src, dst) in enumerate(trio)])
            for copy in loads[-1]:
                copy.start()

    for k, part in enumerate(DENSE_CHUNKS):
        dense_own(x, 0, k, part, to_y)
        dense_own(1 - x, 1, k, part, to_z)

    skip = 192 if first is None else 96
    for k, (start, size) in enumerate(DENSE_CHUNKS):
        if start < skip:
            part = (start, min(skip - start, size))
            dense_own(1 - x, 4, k, part, to_y)
            dense_own(x, 5, k, part, to_z)

    def down_send(p, l):
        rows = pl.ds(p * PIECE, PIECE)
        return remote(down.at[l, rows], w2buf.at[stage * LAYERS + l],
                      ws.at[p, l], wr.at[stage, l], (expert, p))

    def down_arrival(s, l):
        return remote(w2buf.at[s * LAYERS + l], w2buf.at[s * LAYERS + l],
                      ws.at[0, l], wr.at[s, l], to_p)

    def abroad(index):
        return jnp.logical_or(stage != expert, index != expert)

    for l in (0,):
        for p in range(PIECES):
            @pl.when(abroad(p))
            def _():
                down_send(p, l).start()

    def cut_out(l, i, p, r):
        at = pl.ds(i * PACK_ROWS, PACK_ROWS)
        return pltpu.make_async_copy(cut.at[l, p, at], parts[l][r].at[at], outs.at[l, i, p])

    piece = [lax.rem(ids[h], PIECES) for h in range(HOT)]

    def pick(h, units):
        best = units[0]
        for p in range(1, PIECES):
            best = jnp.where(piece[h] == p, units[p], best)
        return best

    for l in range(LAYERS):
        for i in range(PACK_STEPS):
            for copy in loads[l * PACK_STEPS + i]:
                copy.wait()

            def rows13(j):
                start = pl.multiple_of(i * PACK_ROWS + j * SUB_ROWS, SUB_ROWS)
                at = pl.ds(start, SUB_ROWS)
                units = []
                for p in range(PIECES):
                    lo, hi = p * PIECE, (p + 1) * PIECE
                    units.append(jnp.concatenate([gin[l, at, lo:hi], uin[l, at, lo:hi]], axis=-1))
                    cut[l, p, at, :] = units[p]
                for h in range(HOT):
                    unit = pick(h, units)
                    for b in range(3):
                        hot[l, h, pl.ds(b * HIDDEN + start, SUB_ROWS), :] = unit[:, b * LANES:(b + 1) * LANES]

            loop(PACK_ROWS // SUB_ROWS, rows13)
            for b in range(i * PACK_ROWS // LANES, (i + 1) * PACK_ROWS // LANES):
                def rows2(j, b=b):
                    start = pl.multiple_of(j * SUB_ROWS, SUB_ROWS)
                    units = [din[l, pl.ds(p * PIECE + start, SUB_ROWS), b * LANES:(b + 1) * LANES]
                             for p in range(PIECES)]
                    for h in range(HOT):
                        hot[l, h, pl.ds(HOT13 + b * PIECE + start, SUB_ROWS), :] = pick(h, units)

                loop(PIECE // SUB_ROWS, rows2)
            for here in range(STAGES):
                @pl.when(stage == here)
                def _():
                    for p in range(PIECES):
                        cut_out(l, i, p, (p - here) % PIECES).start()

    held = range(HOT) if first is None else ((x + first) % 2,)
    swap = [remote(hot.at[1 - c, h], pbuf.at[h], es.at[n], er.at[n], to_p) for n, h in enumerate(held)]
    for copy in swap:
        copy.start()

    def choose(h, here, mine, other):
        def rows(i):
            at = pl.ds(pl.multiple_of(i * 512, 512), 512)
            ours[h, at, :] = jnp.where(here, mine[h, at, :], other[h, at, :])

        loop(HOT_ROWS // 512, rows)

    landing = xbuf if first is None else ours
    cross = [remote(ours.at[h], landing.at[h], es.at[2 + n], er.at[2 + n], to_x) for n, h in enumerate(held)]
    for n, h in enumerate(held):
        swap[n].wait_recv()
        choose(h, lax.shift_right_logical(ids[h], 2) == expert, hot.at[c], pbuf)
        cross[n].start()

    def relay(k):
        dense_arrival(0, k).wait_recv()
        dense_on(0, 3, k, to_z)
        dense_on(0, 4, k, to_x, skip)
        dense_on(0, 6, k, to_p)
        dense_arrival(1, k).wait_recv()
        dense_on(1, 2, k, to_y)
        dense_on(1, 5, k, to_x, skip)
        dense_on(1, 7, k, to_p)

    half_way = len(DENSE_CHUNKS) // 2 + 1
    for k in range(half_way):
        relay(k)
    for n, h in enumerate(held):
        cross[n].wait()
        if first is None:
            choose(h, lax.shift_right_logical(ids[h], 3) == x, ours, xbuf)
    keep = [pltpu.make_async_copy(ours.at[h], hotf.at[stage, h, c], ls.at[h]) for h in range(HOT)]
    give = [remote(ours.at[h], hotf.at[stage, h, c], es.at[4 + h], er.at[4 + h], to_p) for h in range(HOT)]
    for h in range(HOT):
        keep[h].start()
        give[h].start()

    def hot_own(k):
        at = pl.ds(pl.multiple_of(k * HOT_CHUNK, HOT_CHUNK), HOT_CHUNK)
        hot_send(ours.at[x, at], hot_rows(stage, x, c, k), 0, k, to_y).start()
        hot_send(ours.at[1 - x, at], hot_rows(stage, 1 - x, c, k), 1, k, to_z).start()

    loop(HOT_CHUNKS, hot_own)
    for k in range(half_way, len(DENSE_CHUNKS)):
        relay(k)

    def hot_relay(k):
        hot_arrival(0, k).wait_recv()
        hot_on(0, 3, k, to_z).start()
        hot_on(0, 4, k, to_x).start()
        hot_on(0, 6, k, to_p).start()
        hot_arrival(1, k).wait_recv()
        hot_on(1, 2, k, to_y).start()
        hot_on(1, 5, k, to_x).start()
        hot_on(1, 7, k, to_p).start()

    loop(HOT_CHUNKS, hot_relay)

    for l in (1,):
        for p in range(PIECES):
            @pl.when(abroad(p))
            def _():
                down_send(p, l).start()

    def dense_last(k):
        for i in (4, 5, 2, 3):
            dense_arrival(i, k).wait_recv()
            dense_on(i, 6 + i, k, to_p)

    for k in range(len(DENSE_CHUNKS)):
        dense_last(k)

    def hot_last(k):
        for i in (4, 5, 2, 3):
            hot_arrival(i, k).wait_recv()
            hot_on(i, 6 + i, k, to_p).start()

    loop(HOT_CHUNKS, hot_last)

    def dense_end(k):
        for i in range(12):
            if i >= 6:
                dense_arrival(i, k).wait_recv()
            dense_arrival(i, k).wait_send()

    def hot_end(k):
        for i in range(12):
            if i >= 6:
                hot_arrival(i, k).wait_recv()
            hot_arrival(i, k).wait_send()

    for k in range(len(DENSE_CHUNKS)):
        dense_end(k)
    loop(HOT_CHUNKS, hot_end)
    for copy in swap:
        copy.wait_send()
    for h in range(HOT):
        keep[h].wait()
        give[h].wait()
    for l in range(LAYERS):
        for p in range(PIECES):
            for i in range(PACK_STEPS):
                cut_out(l, i, p, 0).wait()

            @pl.when(abroad(p))
            def _():
                down_send(p, l).wait_send()

            @pl.when(abroad(p))
            def _():
                down_arrival(p, l).wait_recv()


def spread(first, dense, gate, up, down, hot_ids):
    sem = pltpu.SemaphoreType.DMA
    total = STAGES * LAYERS
    return pl.pallas_call(
        functools.partial(spread_kernel, first),
        out_shape=[
            jax.ShapeDtypeStruct((STAGES * 4096, DENSE), BF16),
            jax.ShapeDtypeStruct((STAGES, HOT, LAYERS, HOT_ROWS, LANES), BF16),
            jax.ShapeDtypeStruct((total, PIECE, HIDDEN), BF16),
        ] + [jax.ShapeDtypeStruct((HIDDEN, 2 * PIECE), BF16)] * (LAYERS * PIECES),
        in_specs=[ANY] * 4 + [SMEM],
        out_specs=[ANY] * (3 + LAYERS * PIECES),
        scratch_shapes=[
            pltpu.VMEM((LAYERS, HIDDEN, WIDTH), BF16), pltpu.VMEM((LAYERS, HIDDEN, WIDTH), BF16),
            pltpu.VMEM((LAYERS, WIDTH, HIDDEN), BF16),
            pltpu.VMEM((LAYERS, PIECES, HIDDEN, 2 * PIECE), BF16),
            pltpu.VMEM((LAYERS, HOT, HOT_ROWS, LANES), BF16),
            pltpu.VMEM((HOT, HOT_ROWS, LANES), BF16), pltpu.VMEM((HOT, HOT_ROWS, LANES), BF16),
            pltpu.VMEM((HOT, HOT_ROWS, LANES), BF16),
            sem((12, len(DENSE_CHUNKS))), sem((12, len(DENSE_CHUNKS))),
            sem((12, HOT_CHUNKS)), sem((12, HOT_CHUNKS)),
            sem((6,)), sem((6,)), sem((2,)),
            sem((3 * LAYERS * PACK_STEPS,)), sem((LAYERS, PACK_STEPS, PIECES)),
            sem((PIECES, LAYERS)), sem((STAGES, LAYERS)),
        ],
        compiler_params=pltpu.CompilerParams(has_side_effects=True, vmem_limit_bytes=58 << 20),
        cost_estimate=pl.CostEstimate(flops=1 << 32, bytes_accessed=256 << 20, transcendentals=0),
        name="spread" if first is None else f"spread_{first}",
    )(dense, gate, up, down, hot_ids)


COPY_ROWS = 256
COPY_SLOTS = 12


def dense_copy_kernel(pos, dense, full, out, buf, rs, ws):
    count = STAGES * 4096 // COPY_ROWS
    per_stage = 4096 // COPY_ROWS
    stage = pos[0]

    def rows(k):
        return pl.ds(pl.multiple_of(k * COPY_ROWS, COPY_ROWS), COPY_ROWS)

    def read(k, ref, at):
        slot = lax.rem(k, COPY_SLOTS)
        return pltpu.make_async_copy(ref.at[rows(at)], buf.at[slot], rs.at[slot])

    def write(k):
        slot = lax.rem(k, COPY_SLOTS)
        return pltpu.make_async_copy(buf.at[slot], out.at[rows(k)], ws.at[slot])

    def start(k):
        mine = k // per_stage == stage

        @pl.when(mine)
        def _():
            read(k, dense, k - stage * per_stage).start()

        @pl.when(jnp.logical_not(mine))
        def _():
            read(k, full, k).start()

    ahead = COPY_SLOTS // 2
    loop(ahead, start)

    def step(k):
        @pl.when(k + ahead < count)
        def _():
            @pl.when(k + ahead >= COPY_SLOTS)
            def _():
                write(k + ahead - COPY_SLOTS).wait()

            start(k + ahead)

        read(k, full, k).wait()
        write(k).start()

    loop(count, step)
    loop(COPY_SLOTS, lambda k: write(count - COPY_SLOTS + k).wait())


def dense_copy(stage, dense, full):
    return pl.pallas_call(
        dense_copy_kernel,
        out_shape=jax.ShapeDtypeStruct((STAGES * 4096, DENSE), BF16),
        in_specs=[SMEM, ANY, ANY],
        out_specs=ANY,
        scratch_shapes=[
            pltpu.VMEM((COPY_SLOTS, COPY_ROWS, DENSE), BF16),
            pltpu.SemaphoreType.DMA((COPY_SLOTS,)), pltpu.SemaphoreType.DMA((COPY_SLOTS,)),
        ],
        compiler_params=pltpu.CompilerParams(vmem_limit_bytes=48 << 20),
        cost_estimate=pl.CostEstimate(flops=1 << 28, bytes_accessed=256 << 20, transcendentals=0),
        name="dense_copy",
    )(stage, dense, full)


def spare_kernel(slot, hotf, out13, out2, b13, b2, rs, ws):
    pick = slot[0]
    total = STAGES * LAYERS

    def reads(n, h):
        src = hotf.at[n // LAYERS, h, n % LAYERS]
        for b in range(3):
            yield pltpu.make_async_copy(
                src.at[pl.ds(b * HIDDEN, HIDDEN)], b13.at[n, :, pl.ds(b * LANES, LANES)], rs.at[n])
        for b in range(16):
            yield pltpu.make_async_copy(
                src.at[pl.ds(HOT13 + b * PIECE, PIECE)], b2.at[n, :, pl.ds(b * LANES, LANES)], rs.at[n])

    @pl.when(pick >= 0)
    def _():
        for n in range(total):
            for copy in reads(n, jnp.maximum(pick, 0)):
                copy.start()

    @pl.when(pick < 0)
    def _():
        for n in range(total):
            b13[n] = jnp.zeros((HIDDEN, 2 * PIECE), BF16)
            b2[n] = jnp.zeros((PIECE, HIDDEN), BF16)

    writes = []
    for n in range(total):
        @pl.when(pick >= 0)
        def _():
            pltpu.make_async_copy(out13.at[n], b13.at[n], rs.at[n]).wait()
            pltpu.make_async_copy(out2.at[n], b2.at[n], rs.at[n]).wait()

        writes.append(pltpu.make_async_copy(b13.at[n], out13.at[n], ws.at[n]))
        writes.append(pltpu.make_async_copy(b2.at[n], out2.at[n], ws.at[total + n]))
        writes[-2].start()
        writes[-1].start()
    for copy in writes:
        copy.wait()


def spare(slot, hotf):
    total = STAGES * LAYERS
    return pl.pallas_call(
        spare_kernel,
        out_shape=[
            jax.ShapeDtypeStruct((total, HIDDEN, 2 * PIECE), BF16),
            jax.ShapeDtypeStruct((total, PIECE, HIDDEN), BF16),
        ],
        in_specs=[SMEM, ANY],
        out_specs=[ANY, ANY],
        scratch_shapes=[
            pltpu.VMEM((total, HIDDEN, 2 * PIECE), BF16),
            pltpu.VMEM((total, PIECE, HIDDEN), BF16),
            pltpu.SemaphoreType.DMA((total,)), pltpu.SemaphoreType.DMA((2 * total,)),
        ],
        compiler_params=pltpu.CompilerParams(vmem_limit_bytes=48 << 20),
        cost_estimate=pl.CostEstimate(flops=1 << 26, bytes_accessed=36 << 20, transcendentals=0),
        name="spare",
    )(slot, hotf)


def place2_kernel(pos, down, w2buf, out, buf, rs, ws):
    stage, column = pos[0], pos[1]
    total = STAGES * LAYERS
    own = pl.ds(pl.multiple_of(column * PIECE, PIECE), PIECE)
    for n in range(total):
        mine = jnp.logical_and(stage == column, stage == n // LAYERS)

        @pl.when(mine)
        def _():
            pltpu.make_async_copy(down.at[n % LAYERS, own], buf.at[n], rs.at[n]).start()

        @pl.when(jnp.logical_not(mine))
        def _():
            pltpu.make_async_copy(w2buf.at[n], buf.at[n], rs.at[n]).start()

    writes = [pltpu.make_async_copy(buf.at[n], out.at[n], ws.at[n]) for n in range(total)]
    for n in range(total):
        pltpu.make_async_copy(w2buf.at[n], buf.at[n], rs.at[n]).wait()
        writes[n].start()
    for write in writes:
        write.wait()


def place2(pos, down, w2buf):
    total = STAGES * LAYERS
    return pl.pallas_call(
        place2_kernel,
        out_shape=jax.ShapeDtypeStruct((total, PIECE, HIDDEN), BF16),
        in_specs=[SMEM, ANY, ANY],
        out_specs=ANY,
        scratch_shapes=[
            pltpu.VMEM((total, PIECE, HIDDEN), BF16),
            pltpu.SemaphoreType.DMA((total,)), pltpu.SemaphoreType.DMA((total,)),
        ],
        compiler_params=pltpu.CompilerParams(vmem_limit_bytes=48 << 20),
        cost_estimate=pl.CostEstimate(flops=1 << 25, bytes_accessed=12 << 20, transcendentals=0),
        name="place2",
    )(pos, down, w2buf)


def place13_kernel(layer, rounds, pos, *refs):
    count = len(rounds)
    moved, own, (out, buf, rs, ws) = refs[:count], refs[count], refs[-4:]
    stage, column = pos[0], pos[1]
    for i, r in enumerate(rounds):
        if r == 0:
            @pl.when(stage == column)
            def _():
                pltpu.make_async_copy(own, buf.at[i], rs.at[i]).start()

            @pl.when(stage != column)
            def _():
                pltpu.make_async_copy(moved[i], buf.at[i], rs.at[i]).start()
        else:
            pltpu.make_async_copy(moved[i], buf.at[i], rs.at[i]).start()
    writes = []
    for i, r in enumerate(rounds):
        n = lax.rem(column - r + PIECES, PIECES) * LAYERS + layer
        writes.append(pltpu.make_async_copy(buf.at[i], out.at[n], ws.at[i]))
    for i in range(count):
        pltpu.make_async_copy(moved[i], buf.at[i], rs.at[i]).wait()
        writes[i].start()
    for write in writes:
        write.wait()


def place13(layer, rounds, pos, moved, own, out=None):
    count = len(rounds)
    operands = [pos, *[moved[r] for r in rounds], own] + ([] if out is None else [out])
    return pl.pallas_call(
        functools.partial(place13_kernel, layer, rounds),
        out_shape=jax.ShapeDtypeStruct((STAGES * LAYERS, HIDDEN, 2 * PIECE), BF16),
        in_specs=[SMEM] + [ANY] * (len(operands) - 1),
        out_specs=ANY,
        scratch_shapes=[
            pltpu.VMEM((count, HIDDEN, 2 * PIECE), BF16),
            pltpu.SemaphoreType.DMA((count,)), pltpu.SemaphoreType.DMA((count,)),
        ],
        input_output_aliases={} if out is None else {len(operands) - 1: 0},
        compiler_params=pltpu.CompilerParams(vmem_limit_bytes=48 << 20),
        cost_estimate=pl.CostEstimate(flops=1 << 25, bytes_accessed=count * 3 << 20, transcendentals=0),
        name=f"place13_{layer}{rounds[0]}",
    )(*operands)


def solution(mesh):
    flat_axes = ('stage', 'expert')

    def pairs(r):
        every = [(s * 4 + e, e * 4 + (s + r) % 4) for s in range(4) for e in range(4)]
        return [pair for pair in every if pair[0] != pair[1]]

    def local_move(w_gate, w_up, w_down, dense, hot_ids, spare_map):
        stage = lax.axis_index('stage').astype(jnp.int32)[None]
        column = lax.axis_index('expert').astype(jnp.int32)[None]
        pos = jnp.concatenate([stage, column])
        dense, w_down = dense.reshape(4096, DENSE), w_down[:, 0]
        holders = jnp.sum(lax.shift_right_logical(hot_ids, 3) * (1 + lax.iota(jnp.int32, HOT)))
        case = lax.rem(holders, 3)
        full, hotf, w2buf, *parts = lax.switch(
            case, [functools.partial(spread, first) for first in (None, 1, 0)],
            dense, w_gate[:, 0], w_up[:, 0], w_down, hot_ids)
        moved = [lax.ppermute(part, flat_axes, pairs(i % 4)) for i, part in enumerate(parts)]
        dense_out = dense_copy(stage, dense, full).reshape(STAGES * LAYERS, HIDDEN, DENSE)
        spare13, spare2 = spare(spare_map, hotf)
        w2 = place2(pos, w_down, w2buf)
        w13 = place13(0, (0, 1, 2, 3), pos, moved[:4], parts[0])
        w13 = place13(1, (0, 1), pos, moved[4:], parts[4], w13)
        w13 = place13(1, (2, 3), pos, moved[4:], parts[4], w13)
        return w13[:, None], w2[:, None], dense_out, spare13[:, None], spare2[:, None]

    expert_spec = P('stage', 'expert', None, None)
    unit_spec = P(None, flat_axes, None, None)
    return jax.shard_map(
        local_move,
        mesh=mesh,
        in_specs=(expert_spec, expert_spec, expert_spec, P('stage', None, None), P(None), P(flat_axes)),
        out_specs=(unit_spec, unit_spec, P(None, None, None), unit_spec, unit_spec),
        check_vma=False,
    )
```

```python
import functools

import jax
import jax.numpy as jnp
from jax import lax
from jax.experimental import pallas as pl
from jax.experimental.pallas import tpu as pltpu
from jax.sharding import PartitionSpec as P


MESH = pl.DeviceIdType.MESH
ANY = pl.BlockSpec(memory_space=pl.ANY)
SMEM = pl.BlockSpec(memory_space=pltpu.SMEM)
BF16 = jnp.bfloat16

LAYERS, HIDDEN, WIDTH, DENSE = 2, 2048, 768, 4096
PIECES, PIECE = 4, 192
STAGES = 4
HOT = 2
LANES = 128
HOT13 = 3 * HIDDEN
HOT_ROWS = HOT13 + 16 * PIECE
DENSE_CHUNKS = ((0, 128), (128, 192), (320, 320), (640, 384))
HOT_CHUNKS = 1
HOT_CHUNK = HOT_ROWS // HOT_CHUNKS
PACK_STEPS = 4
PACK_ROWS = HIDDEN // PACK_STEPS
SUB_ROWS = 64


def loop(count, body):
    def step(k, carry):
        body(k)
        return carry

    lax.fori_loop(0, count, step, 0)


def spread_kernel(first, dense, gate, up, down, ids, full, hotf, w2buf, *refs):
    parts, refs = [refs[:4], refs[4:8]], refs[8:]
    gin, uin, din, cut, hot, pbuf, ours, xbuf = refs[:8]
    ds, dr, hs, hr, es, er, ls, ins, outs, ws, wr = refs[8:]
    stage, expert = lax.axis_index('stage'), lax.axis_index('expert')
    z, y = stage // 2, stage % 2
    x, c = expert // 2, expert % 2
    to_y = (z * 2 + 1 - y, expert)
    to_z = ((1 - z) * 2 + y, expert)
    to_x = (stage, (1 - x) * 2 + c)
    to_p = (stage, x * 2 + 1 - c)
    at_y, at_z, at_yz = z * 2 + 1 - y, (1 - z) * 2 + y, (1 - z) * 2 + 1 - y
    flows = [(at_y, x), (at_z, 1 - x), (at_yz, 1 - x), (at_yz, x), (at_y, 1 - x), (at_z, x)]

    def remote(src, dst, send, recv, to):
        return pltpu.make_async_remote_copy(
            src_ref=src, dst_ref=dst, send_sem=send, recv_sem=recv, device_id=to, device_id_type=MESH)

    def part_of(k, skip=0):
        start, size = DENSE_CHUNKS[k]
        cut = max(start, min(skip, start + size))
        return cut, start + size - cut

    def dense_rows(st, half, core, part):
        start = st * 4096 + half * 2048 + core * 1024 + part[0]
        return full.at[pl.ds(pl.multiple_of(start, 32), part[1])]

    def hot_rows(st, half, core, k):
        return hotf.at[st, half, core, pl.ds(pl.multiple_of(k * HOT_CHUNK, HOT_CHUNK), HOT_CHUNK)]

    def dense_send(src, dst, flow, k, to):
        return remote(src, dst, ds.at[flow, k], dr.at[flow, k], to)

    def hot_send(src, dst, flow, k, to):
        return remote(src, dst, hs.at[flow, k], hr.at[flow, k], to)

    def dense_own(half, flow, k, part, to):
        start = half * 2048 + c * 1024 + part[0]
        src = dense.at[pl.ds(pl.multiple_of(start, 32), part[1])]
        dense_send(src, dense_rows(stage, half, c, part), flow, k, to).start()

    def dense_on(i, flow, k, to, skip=0):
        part = part_of(k, skip)
        if part[1]:
            ref = dense_rows(*flows[i], c, part)
            dense_send(ref, ref, flow, k, to).start()

    def hot_on(i, flow, k, to):
        ref = hot_rows(*flows[i], c, k)
        return hot_send(ref, ref, flow, k, to)

    def dense_arrival(flow, k):
        ref = dense_rows(*flows[flow % 6], c if flow < 6 else 1 - c, DENSE_CHUNKS[k])
        return dense_send(ref, ref, flow, k, to_p)

    def hot_arrival(flow, k):
        ref = hot_rows(*flows[flow % 6], c if flow < 6 else 1 - c, k)
        return hot_send(ref, ref, flow, k, to_p)

    for k, part in enumerate(DENSE_CHUNKS):
        dense_own(x, 0, k, part, to_y)
        dense_own(1 - x, 1, k, part, to_z)

    skip = 192 if first is None else 96
    for k, (start, size) in enumerate(DENSE_CHUNKS):
        if start < skip:
            part = (start, min(skip - start, size))
            dense_own(1 - x, 4, k, part, to_y)
            dense_own(x, 5, k, part, to_z)

    loads = []
    for l in range(LAYERS):
        for i in range(PACK_STEPS):
            at = pl.ds(i * PACK_ROWS, PACK_ROWS)
            trio = ((gate.at[l, at], gin.at[l, at]), (up.at[l, at], uin.at[l, at]),
                    (down.at[l, :, at], din.at[l, :, at]))
            loads.append([
                pltpu.make_async_copy(src, dst, ins.at[3 * (l * PACK_STEPS + i) + n])
                for n, (src, dst) in enumerate(trio)])
            for copy in loads[-1]:
                copy.start()

    def down_send(p, l):
        rows = pl.ds(p * PIECE, PIECE)
        return remote(down.at[l, rows], w2buf.at[stage * LAYERS + l],
                      ws.at[p, l], wr.at[stage, l], (expert, p))

    def down_arrival(s, l):
        return remote(w2buf.at[s * LAYERS + l], w2buf.at[s * LAYERS + l],
                      ws.at[0, l], wr.at[s, l], to_p)

    def abroad(index):
        return jnp.logical_or(stage != expert, index != expert)

    for l in (0,):
        for p in range(PIECES):
            @pl.when(abroad(p))
            def _():
                down_send(p, l).start()

    def cut_out(l, i, p, r):
        at = pl.ds(i * PACK_ROWS, PACK_ROWS)
        return pltpu.make_async_copy(cut.at[l, p, at], parts[l][r].at[at], outs.at[l, i, p])

    piece = [lax.rem(ids[h], PIECES) for h in range(HOT)]

    def pick(h, units):
        best = units[0]
        for p in range(1, PIECES):
            best = jnp.where(piece[h] == p, units[p], best)
        return best

    for l in range(LAYERS):
        for i in range(PACK_STEPS):
            for copy in loads[l * PACK_STEPS + i]:
                copy.wait()

            def rows13(j):
                start = pl.multiple_of(i * PACK_ROWS + j * SUB_ROWS, SUB_ROWS)
                at = pl.ds(start, SUB_ROWS)
                units = []
                for p in range(PIECES):
                    lo, hi = p * PIECE, (p + 1) * PIECE
                    units.append(jnp.concatenate([gin[l, at, lo:hi], uin[l, at, lo:hi]], axis=-1))
                    cut[l, p, at, :] = units[p]
                for h in range(HOT):
                    unit = pick(h, units)
                    for b in range(3):
                        hot[l, h, pl.ds(b * HIDDEN + start, SUB_ROWS), :] = unit[:, b * LANES:(b + 1) * LANES]

            loop(PACK_ROWS // SUB_ROWS, rows13)
            for b in range(i * PACK_ROWS // LANES, (i + 1) * PACK_ROWS // LANES):
                def rows2(j, b=b):
                    start = pl.multiple_of(j * SUB_ROWS, SUB_ROWS)
                    units = [din[l, pl.ds(p * PIECE + start, SUB_ROWS), b * LANES:(b + 1) * LANES]
                             for p in range(PIECES)]
                    for h in range(HOT):
                        hot[l, h, pl.ds(HOT13 + b * PIECE + start, SUB_ROWS), :] = pick(h, units)

                loop(PIECE // SUB_ROWS, rows2)
            for here in range(STAGES):
                @pl.when(stage == here)
                def _():
                    for p in range(PIECES):
                        cut_out(l, i, p, (p - here) % PIECES).start()

    held = range(HOT) if first is None else ((x + first) % 2,)
    swap = [remote(hot.at[1 - c, h], pbuf.at[h], es.at[n], er.at[n], to_p) for n, h in enumerate(held)]
    for copy in swap:
        copy.start()

    def choose(h, here, mine, other):
        def rows(i):
            at = pl.ds(pl.multiple_of(i * 512, 512), 512)
            ours[h, at, :] = jnp.where(here, mine[h, at, :], other[h, at, :])

        loop(HOT_ROWS // 512, rows)

    landing = xbuf if first is None else ours
    cross = [remote(ours.at[h], landing.at[h], es.at[2 + n], er.at[2 + n], to_x) for n, h in enumerate(held)]
    for n, h in enumerate(held):
        swap[n].wait_recv()
        choose(h, lax.shift_right_logical(ids[h], 2) == expert, hot.at[c], pbuf)
        cross[n].start()

    def relay(k):
        dense_arrival(0, k).wait_recv()
        dense_on(0, 3, k, to_z)
        dense_on(0, 4, k, to_x, skip)
        dense_on(0, 6, k, to_p)
        dense_arrival(1, k).wait_recv()
        dense_on(1, 2, k, to_y)
        dense_on(1, 5, k, to_x, skip)
        dense_on(1, 7, k, to_p)

    half_way = len(DENSE_CHUNKS) // 2 + 1
    for k in range(half_way):
        relay(k)
    for n, h in enumerate(held):
        cross[n].wait()
        if first is None:
            choose(h, lax.shift_right_logical(ids[h], 3) == x, ours, xbuf)
    keep = [pltpu.make_async_copy(ours.at[h], hotf.at[stage, h, c], ls.at[h]) for h in range(HOT)]
    give = [remote(ours.at[h], hotf.at[stage, h, c], es.at[4 + h], er.at[4 + h], to_p) for h in range(HOT)]
    for h in range(HOT):
        keep[h].start()
        give[h].start()

    def hot_own(k):
        at = pl.ds(pl.multiple_of(k * HOT_CHUNK, HOT_CHUNK), HOT_CHUNK)
        hot_send(ours.at[x, at], hot_rows(stage, x, c, k), 0, k, to_y).start()
        hot_send(ours.at[1 - x, at], hot_rows(stage, 1 - x, c, k), 1, k, to_z).start()

    loop(HOT_CHUNKS, hot_own)
    for k in range(half_way, len(DENSE_CHUNKS)):
        relay(k)

    def hot_relay(k):
        hot_arrival(0, k).wait_recv()
        hot_on(0, 3, k, to_z).start()
        hot_on(0, 4, k, to_x).start()
        hot_on(0, 6, k, to_p).start()
        hot_arrival(1, k).wait_recv()
        hot_on(1, 2, k, to_y).start()
        hot_on(1, 5, k, to_x).start()
        hot_on(1, 7, k, to_p).start()

    loop(HOT_CHUNKS, hot_relay)

    for l in (1,):
        for p in range(PIECES):
            @pl.when(abroad(p))
            def _():
                down_send(p, l).start()

    def dense_last(k):
        for i in (4, 5, 2, 3):
            dense_arrival(i, k).wait_recv()
            dense_on(i, 6 + i, k, to_p)

    for k in range(len(DENSE_CHUNKS)):
        dense_last(k)

    def hot_last(k):
        for i in (4, 5, 2, 3):
            hot_arrival(i, k).wait_recv()
            hot_on(i, 6 + i, k, to_p).start()

    loop(HOT_CHUNKS, hot_last)

    def dense_end(k):
        for i in range(12):
            if i >= 6:
                dense_arrival(i, k).wait_recv()
            dense_arrival(i, k).wait_send()

    def hot_end(k):
        for i in range(12):
            if i >= 6:
                hot_arrival(i, k).wait_recv()
            hot_arrival(i, k).wait_send()

    for k in range(len(DENSE_CHUNKS)):
        dense_end(k)
    loop(HOT_CHUNKS, hot_end)
    for copy in swap:
        copy.wait_send()
    for h in range(HOT):
        keep[h].wait()
        give[h].wait()
    for l in range(LAYERS):
        for p in range(PIECES):
            for i in range(PACK_STEPS):
                cut_out(l, i, p, 0).wait()

            @pl.when(abroad(p))
            def _():
                down_send(p, l).wait_send()

            @pl.when(abroad(p))
            def _():
                down_arrival(p, l).wait_recv()


def spread(first, dense, gate, up, down, hot_ids):
    sem = pltpu.SemaphoreType.DMA
    total = STAGES * LAYERS
    return pl.pallas_call(
        functools.partial(spread_kernel, first),
        out_shape=[
            jax.ShapeDtypeStruct((STAGES * 4096, DENSE), BF16),
            jax.ShapeDtypeStruct((STAGES, HOT, LAYERS, HOT_ROWS, LANES), BF16),
            jax.ShapeDtypeStruct((total, PIECE, HIDDEN), BF16),
        ] + [jax.ShapeDtypeStruct((HIDDEN, 2 * PIECE), BF16)] * (LAYERS * PIECES),
        in_specs=[ANY] * 4 + [SMEM],
        out_specs=[ANY] * (3 + LAYERS * PIECES),
        scratch_shapes=[
            pltpu.VMEM((LAYERS, HIDDEN, WIDTH), BF16), pltpu.VMEM((LAYERS, HIDDEN, WIDTH), BF16),
            pltpu.VMEM((LAYERS, WIDTH, HIDDEN), BF16),
            pltpu.VMEM((LAYERS, PIECES, HIDDEN, 2 * PIECE), BF16),
            pltpu.VMEM((LAYERS, HOT, HOT_ROWS, LANES), BF16),
            pltpu.VMEM((HOT, HOT_ROWS, LANES), BF16), pltpu.VMEM((HOT, HOT_ROWS, LANES), BF16),
            pltpu.VMEM((HOT, HOT_ROWS, LANES), BF16),
            sem((12, len(DENSE_CHUNKS))), sem((12, len(DENSE_CHUNKS))),
            sem((12, HOT_CHUNKS)), sem((12, HOT_CHUNKS)),
            sem((6,)), sem((6,)), sem((2,)),
            sem((3 * LAYERS * PACK_STEPS,)), sem((LAYERS, PACK_STEPS, PIECES)),
            sem((PIECES, LAYERS)), sem((STAGES, LAYERS)),
        ],
        compiler_params=pltpu.CompilerParams(has_side_effects=True, vmem_limit_bytes=58 << 20),
        cost_estimate=pl.CostEstimate(flops=1 << 32, bytes_accessed=256 << 20, transcendentals=0),
        name="spread" if first is None else f"spread_{first}",
    )(dense, gate, up, down, hot_ids)


COPY_ROWS = 256
COPY_SLOTS = 12


def dense_copy_kernel(pos, dense, full, out, buf, rs, ws):
    count = STAGES * 4096 // COPY_ROWS
    per_stage = 4096 // COPY_ROWS
    stage = pos[0]

    def rows(k):
        return pl.ds(pl.multiple_of(k * COPY_ROWS, COPY_ROWS), COPY_ROWS)

    def read(k, ref, at):
        slot = lax.rem(k, COPY_SLOTS)
        return pltpu.make_async_copy(ref.at[rows(at)], buf.at[slot], rs.at[slot])

    def write(k):
        slot = lax.rem(k, COPY_SLOTS)
        return pltpu.make_async_copy(buf.at[slot], out.at[rows(k)], ws.at[slot])

    def start(k):
        mine = k // per_stage == stage

        @pl.when(mine)
        def _():
            read(k, dense, k - stage * per_stage).start()

        @pl.when(jnp.logical_not(mine))
        def _():
            read(k, full, k).start()

    ahead = COPY_SLOTS // 2
    loop(ahead, start)

    def step(k):
        @pl.when(k + ahead < count)
        def _():
            @pl.when(k + ahead >= COPY_SLOTS)
            def _():
                write(k + ahead - COPY_SLOTS).wait()

            start(k + ahead)

        read(k, full, k).wait()
        write(k).start()

    loop(count, step)
    loop(COPY_SLOTS, lambda k: write(count - COPY_SLOTS + k).wait())


def dense_copy(stage, dense, full):
    return pl.pallas_call(
        dense_copy_kernel,
        out_shape=jax.ShapeDtypeStruct((STAGES * 4096, DENSE), BF16),
        in_specs=[SMEM, ANY, ANY],
        out_specs=ANY,
        scratch_shapes=[
            pltpu.VMEM((COPY_SLOTS, COPY_ROWS, DENSE), BF16),
            pltpu.SemaphoreType.DMA((COPY_SLOTS,)), pltpu.SemaphoreType.DMA((COPY_SLOTS,)),
        ],
        compiler_params=pltpu.CompilerParams(vmem_limit_bytes=48 << 20),
        cost_estimate=pl.CostEstimate(flops=1 << 28, bytes_accessed=256 << 20, transcendentals=0),
        name="dense_copy",
    )(stage, dense, full)


def spare_kernel(slot, hotf, out13, out2, b13, b2, rs, ws):
    pick = slot[0]
    total = STAGES * LAYERS

    def reads(n, h):
        src = hotf.at[n // LAYERS, h, n % LAYERS]
        for b in range(3):
            yield pltpu.make_async_copy(
                src.at[pl.ds(b * HIDDEN, HIDDEN)], b13.at[n, :, pl.ds(b * LANES, LANES)], rs.at[n])
        for b in range(16):
            yield pltpu.make_async_copy(
                src.at[pl.ds(HOT13 + b * PIECE, PIECE)], b2.at[n, :, pl.ds(b * LANES, LANES)], rs.at[n])

    @pl.when(pick >= 0)
    def _():
        for n in range(total):
            for copy in reads(n, jnp.maximum(pick, 0)):
                copy.start()

    @pl.when(pick < 0)
    def _():
        for n in range(total):
            b13[n] = jnp.zeros((HIDDEN, 2 * PIECE), BF16)
            b2[n] = jnp.zeros((PIECE, HIDDEN), BF16)

    writes = []
    for n in range(total):
        @pl.when(pick >= 0)
        def _():
            pltpu.make_async_copy(out13.at[n], b13.at[n], rs.at[n]).wait()
            pltpu.make_async_copy(out2.at[n], b2.at[n], rs.at[n]).wait()

        writes.append(pltpu.make_async_copy(b13.at[n], out13.at[n], ws.at[n]))
        writes.append(pltpu.make_async_copy(b2.at[n], out2.at[n], ws.at[total + n]))
        writes[-2].start()
        writes[-1].start()
    for copy in writes:
        copy.wait()


def spare(slot, hotf):
    total = STAGES * LAYERS
    return pl.pallas_call(
        spare_kernel,
        out_shape=[
            jax.ShapeDtypeStruct((total, HIDDEN, 2 * PIECE), BF16),
            jax.ShapeDtypeStruct((total, PIECE, HIDDEN), BF16),
        ],
        in_specs=[SMEM, ANY],
        out_specs=[ANY, ANY],
        scratch_shapes=[
            pltpu.VMEM((total, HIDDEN, 2 * PIECE), BF16),
            pltpu.VMEM((total, PIECE, HIDDEN), BF16),
            pltpu.SemaphoreType.DMA((total,)), pltpu.SemaphoreType.DMA((2 * total,)),
        ],
        compiler_params=pltpu.CompilerParams(vmem_limit_bytes=48 << 20),
        cost_estimate=pl.CostEstimate(flops=1 << 26, bytes_accessed=36 << 20, transcendentals=0),
        name="spare",
    )(slot, hotf)


def place2_kernel(pos, down, w2buf, out, buf, rs, ws):
    stage, column = pos[0], pos[1]
    total = STAGES * LAYERS
    own = pl.ds(pl.multiple_of(column * PIECE, PIECE), PIECE)
    for n in range(total):
        mine = jnp.logical_and(stage == column, stage == n // LAYERS)

        @pl.when(mine)
        def _():
            pltpu.make_async_copy(down.at[n % LAYERS, own], buf.at[n], rs.at[n]).start()

        @pl.when(jnp.logical_not(mine))
        def _():
            pltpu.make_async_copy(w2buf.at[n], buf.at[n], rs.at[n]).start()

    writes = [pltpu.make_async_copy(buf.at[n], out.at[n], ws.at[n]) for n in range(total)]
    for n in range(total):
        pltpu.make_async_copy(w2buf.at[n], buf.at[n], rs.at[n]).wait()
        writes[n].start()
    for write in writes:
        write.wait()


def place2(pos, down, w2buf):
    total = STAGES * LAYERS
    return pl.pallas_call(
        place2_kernel,
        out_shape=jax.ShapeDtypeStruct((total, PIECE, HIDDEN), BF16),
        in_specs=[SMEM, ANY, ANY],
        out_specs=ANY,
        scratch_shapes=[
            pltpu.VMEM((total, PIECE, HIDDEN), BF16),
            pltpu.SemaphoreType.DMA((total,)), pltpu.SemaphoreType.DMA((total,)),
        ],
        compiler_params=pltpu.CompilerParams(vmem_limit_bytes=48 << 20),
        cost_estimate=pl.CostEstimate(flops=1 << 25, bytes_accessed=12 << 20, transcendentals=0),
        name="place2",
    )(pos, down, w2buf)


def place13_kernel(layer, rounds, pos, *refs):
    count = len(rounds)
    moved, own, (out, buf, rs, ws) = refs[:count], refs[count], refs[-4:]
    stage, column = pos[0], pos[1]
    for i, r in enumerate(rounds):
        if r == 0:
            @pl.when(stage == column)
            def _():
                pltpu.make_async_copy(own, buf.at[i], rs.at[i]).start()

            @pl.when(stage != column)
            def _():
                pltpu.make_async_copy(moved[i], buf.at[i], rs.at[i]).start()
        else:
            pltpu.make_async_copy(moved[i], buf.at[i], rs.at[i]).start()
    writes = []
    for i, r in enumerate(rounds):
        n = lax.rem(column - r + PIECES, PIECES) * LAYERS + layer
        writes.append(pltpu.make_async_copy(buf.at[i], out.at[n], ws.at[i]))
    for i in range(count):
        pltpu.make_async_copy(moved[i], buf.at[i], rs.at[i]).wait()
        writes[i].start()
    for write in writes:
        write.wait()


def place13(layer, rounds, pos, moved, own, out=None):
    count = len(rounds)
    operands = [pos, *[moved[r] for r in rounds], own] + ([] if out is None else [out])
    return pl.pallas_call(
        functools.partial(place13_kernel, layer, rounds),
        out_shape=jax.ShapeDtypeStruct((STAGES * LAYERS, HIDDEN, 2 * PIECE), BF16),
        in_specs=[SMEM] + [ANY] * (len(operands) - 1),
        out_specs=ANY,
        scratch_shapes=[
            pltpu.VMEM((count, HIDDEN, 2 * PIECE), BF16),
            pltpu.SemaphoreType.DMA((count,)), pltpu.SemaphoreType.DMA((count,)),
        ],
        input_output_aliases={} if out is None else {len(operands) - 1: 0},
        compiler_params=pltpu.CompilerParams(vmem_limit_bytes=48 << 20),
        cost_estimate=pl.CostEstimate(flops=1 << 25, bytes_accessed=count * 3 << 20, transcendentals=0),
        name=f"place13_{layer}{rounds[0]}",
    )(*operands)


def solution(mesh):
    flat_axes = ('stage', 'expert')

    def pairs(r):
        every = [(s * 4 + e, e * 4 + (s + r) % 4) for s in range(4) for e in range(4)]
        return [pair for pair in every if pair[0] != pair[1]]

    def local_move(w_gate, w_up, w_down, dense, hot_ids, spare_map):
        stage = lax.axis_index('stage').astype(jnp.int32)[None]
        column = lax.axis_index('expert').astype(jnp.int32)[None]
        pos = jnp.concatenate([stage, column])
        dense, w_down = dense.reshape(4096, DENSE), w_down[:, 0]
        holders = jnp.sum(lax.shift_right_logical(hot_ids, 3) * (1 + lax.iota(jnp.int32, HOT)))
        case = lax.rem(holders, 3)
        full, hotf, w2buf, *parts = lax.switch(
            case, [functools.partial(spread, first) for first in (None, 1, 0)],
            dense, w_gate[:, 0], w_up[:, 0], w_down, hot_ids)
        moved = [lax.ppermute(part, flat_axes, pairs(i % 4)) for i, part in enumerate(parts)]
        dense_out = dense_copy(stage, dense, full).reshape(STAGES * LAYERS, HIDDEN, DENSE)
        spare13, spare2 = spare(spare_map, hotf)
        w2 = place2(pos, w_down, w2buf)
        w13 = place13(0, (0, 1, 2, 3), pos, moved[:4], parts[0])
        w13 = place13(1, (0, 1), pos, moved[4:], parts[4], w13)
        w13 = place13(1, (2, 3), pos, moved[4:], parts[4], w13)
        return w13[:, None], w2[:, None], dense_out, spare13[:, None], spare2[:, None]

    expert_spec = P('stage', 'expert', None, None)
    unit_spec = P(None, flat_axes, None, None)
    return jax.shard_map(
        local_move,
        mesh=mesh,
        in_specs=(expert_spec, expert_spec, expert_spec, P('stage', None, None), P(None), P(flat_axes)),
        out_specs=(unit_spec, unit_spec, P(None, None, None), unit_spec, unit_spec),
        check_vma=False,
    )
```
